32 devices in a mesh: stream: 8 (over z, x), span: 4 (over y, core).
Axes of the slice: x: 2, y: 2, z: 4, core: 2. Of those that a mesh axis runs over, the one named last changes fastest.
Arguments:
- state: float32 [320, 8, 625], P('stream', 'span'), may hold values from -0.25 to 2.5, as said below
- direction: float32 [320, 8, 625], P('stream', 'span'), may hold values from -6 to 6
- metric: float32 [320, 8, 3], P('stream', 'span'), may hold values from 1 to 4
- face_source: int32 [320, 4], P('stream'), may hold values from -1 to 225, as said below
- send_rows: int32 [8, 2, 33], P('stream'), may hold values from 0 to 159, as said below
Outputs:
- residual: float32 [320, 8, 625], P('stream', 'span')
- basis_next: float32 [320, 8, 625], P('stream', 'span')
- krylov: float32 [3], replicated
The draws below stay inside these ranges and needn't reach their ends.
Inputs may be any that keep to these rules, and one draw needn't show every extreme that they name: `state`: conserved variables from density 0.75 to 1.25, flow-wise velocity 0.1 to 0.5, other velocities -0.2 to 0.2, pressure 0.5 to 0.9, so pressure and temperature are positive. `face_source`: the plane is a grid of columns of 32 cells, numbered column by column, partition d owning cells d * 40 to (d + 1) * 40 - 1 in a random local order; flow-wise faces wrap around. Every face neighbour lies in the same or an adjacent partition; -1 stands exactly on the lower face of the lowest and the upper face of the highest row; indices into received blocks point at used slots. `send_rows`: at most 33 faces per neighbouring pair, and some pair uses all 33; slots beyond a pair's count hold 0; the order of slots is the order in which the receiver's face_source refers to them.
All inputs are finite; a program needn't handle non-finite values.
Results may differ from the reference program's by a relative error of at most 0.0003.
Values sent between devices are 32-bit elements.
A program may use at most 128 MiB of HBM per device.

```python
import math
import jax
import jax.numpy as jnp
import numpy as np
from jax import lax

COLUMNS = 40
WALL_ROWS = 32
NODES = 125
VARS = 5
SLOTS = 33
PLANE = 320
LAYERS = 8
N_STREAM = 8


GAMMA_RATIO = 1.4


def draw_state(key, part):
    noise_shape = (PLANE, LAYERS, 5, NODES)
    noise = jnp.clip(0.4 * jax.random.normal(key, noise_shape, jnp.float32), -1.0, 1.0)
    density = 1.0 + 0.25 * noise[:, :, 0]
    flow_speed = 0.3 + 0.2 * noise[:, :, 1]
    normal_speed = 0.2 * noise[:, :, 2]
    span_speed = 0.2 * noise[:, :, 3]
    pressure = 0.7 + 0.2 * noise[:, :, 4]
    kinetic = 0.5 * density * (flow_speed * flow_speed + normal_speed * normal_speed + span_speed * span_speed)
    energy = pressure / (GAMMA_RATIO - 1.0) + kinetic
    stacked = jnp.stack([density, density * flow_speed, density * normal_speed, density * span_speed, energy], axis=2)
    return stacked.reshape(PLANE, LAYERS, 5 * NODES)


def mesh_tables(key):
    devices = N_STREAM
    cell_ids = jnp.arange(PLANE, dtype=jnp.int32)
    owner_part = cell_ids // COLUMNS
    position = cell_ids % COLUMNS
    part_keys = jax.random.split(jax.random.fold_in(key, 17), devices)
    orders = jax.vmap(lambda single: jax.random.permutation(single, COLUMNS))(part_keys).astype(jnp.int32)
    local_column = orders[owner_part, position]
    column_count = PLANE // WALL_ROWS
    flow_column = cell_ids // WALL_ROWS
    wall_row = cell_ids % WALL_ROWS
    neighbor = jnp.stack([(flow_column - 1) % column_count * WALL_ROWS + wall_row, (flow_column + 1) % column_count * WALL_ROWS + wall_row, cell_ids - 1, cell_ids + 1], axis=1)
    walled = jnp.stack([wall_row < 0, wall_row < 0, wall_row == 0, wall_row == WALL_ROWS - 1], axis=1)
    neighbor = jnp.where(walled, cell_ids[:, None], neighbor)
    other_owner = neighbor // COLUMNS
    face_ids = jnp.arange(4, dtype=jnp.int32)[None, :]
    to_left = jnp.logical_and(jnp.logical_not(walled), other_owner == (owner_part[:, None] - 1) % devices)
    to_right = jnp.logical_and(jnp.logical_not(walled), other_owner == (owner_part[:, None] + 1) % devices)

    def slots_of(flags):
        flat_flags = flags.reshape(devices, COLUMNS * 4).astype(jnp.int32)
        before = jnp.cumsum(flat_flags, axis=1) - flat_flags
        return before.reshape(PLANE, 4)
    left_slot = slots_of(to_left)
    right_slot = slots_of(to_right)
    own_index = local_column[:, None] * 4 + face_ids
    owners = jnp.broadcast_to(owner_part[:, None], (PLANE, 4))
    send_table = jnp.zeros((devices, 2, SLOTS), jnp.int32)
    send_table = send_table.at[owners, 0, jnp.where(to_left, left_slot, SLOTS)].set(own_index, mode='drop')
    send_table = send_table.at[owners, 1, jnp.where(to_right, right_slot, SLOTS)].set(own_index, mode='drop')
    partner_face = face_ids + 1 - 2 * (face_ids % 2)
    partner_local = local_column[neighbor] * 4 + partner_face
    from_right = COLUMNS * 4 + SLOTS + left_slot[neighbor, partner_face]
    from_left = COLUMNS * 4 + right_slot[neighbor, partner_face]
    source = jnp.where(to_right, from_right, jnp.where(to_left, from_left, partner_local))
    source = jnp.where(walled, -1, source).astype(jnp.int32)
    row_ids = owner_part * COLUMNS + local_column
    source_table = jnp.zeros((PLANE, 4), jnp.int32).at[row_ids].set(source)
    return (source_table, send_table)


def draw_face_source(key, part):
    return mesh_tables(key)[0]


def draw_send_rows(key, part):
    return mesh_tables(key)[1]


def levels(key, shape, pieces, least, high):
    factor_of, own = 1.0, jax.random.fold_in(key, 6)
    for axis_at, shards_of in pieces:
        draws = jnp.exp(jax.random.uniform(jax.random.fold_in(own, axis_at), (shards_of,), jnp.float32, least / len(pieces), high / len(pieces)))
        factor_of = factor_of * jnp.repeat(draws, shape[axis_at] // shards_of).reshape([-1 if axis == axis_at else 1 for axis in range(len(shape))])
    return factor_of


def bell_draw(key, extent, scale, limit, shards=(), held_as=jnp.bfloat16):
    values = scale * jax.random.normal(key, extent, jnp.float32)
    if shards:
        values = values * levels(key, extent, shards, -0.22, 0.18)
    return jnp.clip(values, -limit, limit).astype(held_as)


def setup_inputs(seed: int = 0) -> dict:
    arg_keys = jax.random.split(jax.random.key(seed), 6)
    return {
        "state": draw_state(jax.random.fold_in(arg_keys[5], 71), 0),
        "direction": bell_draw(arg_keys[1], (PLANE, LAYERS, NODES * VARS), 1.0, 6.0, ((0, 8), (1, 4)), jnp.float32),
        "metric": jnp.clip(jnp.exp(math.log(4.0) - 1.3862944 * jax.random.uniform(arg_keys[2], (PLANE, LAYERS, 3), jnp.float32) ** levels(arg_keys[2], (PLANE, LAYERS, 3), ((0, 8), (1, 4)), -0.2, 0.2)), 1.0, 4.0),
        "face_source": draw_face_source(jax.random.fold_in(arg_keys[5], 71), 0),
        "send_rows": draw_send_rows(jax.random.fold_in(arg_keys[5], 71), 0),
    }


GAMMA = 1.4
VISC = 0.01
COND = VISC * GAMMA / ((GAMMA - 1.0) * 0.72)
LIFT = 10.0
EINSUM_FORMS = ('ai,...ijk->...ajk', 'aj,...ijk->...iak', 'ak,...ijk->...ija')

def diff_table():
    spread = math.sqrt(3.0 / 7.0)
    points = np.array([-1.0, -spread, 0.0, spread, 1.0])
    weights = np.array([np.prod([points[row_at] - points[other] for other in range(5) if other != row_at]) for row_at in range(5)])
    matrix = np.zeros((5, 5))
    for row_at in range(5):
        for col_at in range(5):
            if row_at != col_at:
                matrix[row_at, col_at] = weights[row_at] / (weights[col_at] * (points[row_at] - points[col_at]))
        matrix[row_at, row_at] = np.sum([1.0 / (points[row_at] - points[other]) for other in range(5) if other != row_at])
    return matrix

def derivative(field, axis_pick):
    matrix = jnp.asarray(diff_table(), dtype=jnp.float32)
    return jnp.einsum(EINSUM_FORMS[axis_pick], matrix, field, precision=lax.Precision.HIGHEST)

def face_slice(volume, face_index):
    endpoint = 4 * (face_index % 2)
    if face_index < 2:
        return volume[..., endpoint, :, :]
    if face_index < 4:
        return volume[..., :, endpoint, :]
    return volume[..., :, :, endpoint]

def put_face(volume, face_index, values):
    endpoint = 4 * (face_index % 2)
    if face_index < 2:
        return volume.at[..., endpoint, :, :].add(values)
    if face_index < 4:
        return volume.at[..., :, endpoint, :].add(values)
    return volume.at[..., :, :, endpoint].add(values)

def primitive(components):
    density = components[0]
    velocity = [components[1] / density, components[2] / density, components[3] / density]
    kinetic = 0.5 * (components[1] * velocity[0] + components[2] * velocity[1] + components[3] * velocity[2])
    pressure = (GAMMA - 1.0) * (components[4] - kinetic)
    return (velocity, pressure, pressure / density)

def inviscid(components, axis_pick):
    velocity, pressure, temper = primitive(components)
    normal_speed = velocity[axis_pick]
    result = [components[1 + axis_pick]]
    for member in range(3):
        flux_term = components[1 + member] * normal_speed
        if member == axis_pick:
            flux_term = flux_term + pressure
        result.append(flux_term)
    result.append((components[4] + pressure) * normal_speed)
    return result

def viscous(components, gradients, axis_pick):
    velocity, pressure, temper = primitive(components)
    divergence = gradients[0][0] + gradients[1][1] + gradients[2][2]
    stresses = []
    for member in range(3):
        stress = gradients[axis_pick][member] + gradients[member][axis_pick]
        if member == axis_pick:
            stress = stress - 2.0 / 3.0 * divergence
        stresses.append(VISC * stress)
    energy = stresses[0] * velocity[0] + stresses[1] * velocity[1] + stresses[2] * velocity[2] + COND * gradients[axis_pick][3]
    return [jnp.zeros_like(energy)] + stresses + [energy]

def wave_square(components):
    velocity, pressure, temper = primitive(components)
    return velocity[0] * velocity[0] + velocity[1] * velocity[1] + velocity[2] * velocity[2] + GAMMA * temper

def lifted_gradient(volume, outside, scales):
    components = [volume[..., member, :, :, :] for member in range(5)]
    velocity, pressure, temper = primitive(components)
    fields = velocity + [temper]
    outer_fields = []
    for face_index in range(6):
        outer_parts = [outside[face_index][..., member, :, :] for member in range(5)]
        outer_velocity, outer_pressure, outer_temper = primitive(outer_parts)
        outer_fields.append(outer_velocity + [outer_temper])
    gradients = []
    for axis_pick in range(3):
        factor = scales[..., axis_pick][..., None, None, None]
        grad_row = []
        for field_index in range(4):
            accumulated = derivative(fields[field_index], axis_pick)
            for upper_side in range(2):
                face_index = 2 * axis_pick + upper_side
                normal_sign = 2.0 * upper_side - 1.0
                trace_jump = outer_fields[face_index][field_index] - face_slice(fields[field_index], face_index)
                accumulated = put_face(accumulated, face_index, 0.5 * LIFT * normal_sign * trace_jump)
            grad_row.append(factor * accumulated)
        gradients.append(grad_row)
    return gradients

def own_viscous_faces(volume, gradients):
    components = [volume[..., member, :, :, :] for member in range(5)]
    result = []
    for face_index in range(6):
        face_parts = [face_slice(piece, face_index) for piece in components]
        face_grads = [[face_slice(entry, face_index) for entry in grad_row] for grad_row in gradients]
        result.append(jnp.stack(viscous(face_parts, face_grads, face_index // 2), axis=-3))
    return result

def residual_terms(volume, outside, gradients, visc_outside, scales, walls):
    components = [volume[..., member, :, :, :] for member in range(5)]
    totals = [jnp.zeros_like(components[0]) for member in range(5)]
    for axis_pick in range(3):
        factor = scales[..., axis_pick][..., None, None, None]
        convect = inviscid(components, axis_pick)
        diffuse = viscous(components, gradients, axis_pick)
        accumulated = [derivative(convect[member] - diffuse[member], axis_pick) for member in range(5)]
        for upper_side in range(2):
            face_index = 2 * axis_pick + upper_side
            normal_sign = 2.0 * upper_side - 1.0
            inner_parts = [face_slice(piece, face_index) for piece in components]
            outer_parts = [outside[face_index][..., member, :, :] for member in range(5)]
            outer_flux = inviscid(outer_parts, axis_pick)
            speed = jnp.sqrt(0.5 * (wave_square(inner_parts) + wave_square(outer_parts)))
            for member in range(5):
                inner_visc = face_slice(diffuse[member], face_index)
                outer_visc = visc_outside[face_index][..., member, :, :]
                if walls[face_index] is not None:
                    outer_visc = jnp.where(walls[face_index], inner_visc, outer_visc)
                surface = normal_sign * 0.5 * (outer_flux[member] - face_slice(convect[member], face_index)) - 0.5 * speed * (outer_parts[member] - inner_parts[member]) - normal_sign * 0.5 * (outer_visc - inner_visc)
                accumulated[member] = put_face(accumulated[member], face_index, LIFT * surface)
        totals = [totals[member] + factor * accumulated[member] for member in range(5)]
    return jnp.stack(totals, axis=-4)

def wall_masks(face_source):
    masks = [None, None, None, None, None, None]
    for face_index in (2, 3):
        masks[face_index] = (face_source[:, face_index] < 0)[:, None, None, None]
    return masks

def mirrored(face_trace):
    flips = 2.0 * (jnp.arange(5) % 4 == 0).astype(jnp.float32) - 1.0
    return face_trace * flips[:, None, None]

def pack_faces(volume):
    lead_shape = volume.shape[:2] + (-1,)
    return jnp.stack([face_slice(volume, face_index).reshape(lead_shape) for face_index in range(6)], axis=1)

def stack_faces(face_list):
    lead_shape = face_list[0].shape[:2] + (-1,)
    return jnp.stack([entry.reshape(lead_shape) for entry in face_list], axis=1)

def send_buffers(table, send_rows):
    picked = jnp.take(table, send_rows.reshape(-1), axis=0)
    return picked.reshape((2, send_rows.shape[2]) + table.shape[1:])

def pick_outside(table, received, face_source):
    whole = jnp.concatenate([table, received[0], received[3]], axis=0)
    picked = jnp.take(whole, jnp.maximum(face_source, 0).reshape(-1), axis=0)
    return picked.reshape(face_source.shape + table.shape[1:])

def split_traces(outside, upper_half, trailing):
    half_width = outside[0].shape[-1] // 2
    offset = half_width * upper_half
    return [entry[..., offset:offset + half_width].reshape(entry.shape[:-1] + trailing) for entry in outside]

def with_walls(outside, own_volume, walls):
    result = []
    for face_index in range(6):
        face_trace = outside[face_index]
        if walls[face_index] is not None:
            face_trace = jnp.where(walls[face_index][..., None], mirrored(face_slice(own_volume, face_index)), face_trace)
        result.append(face_trace)
    return result

def plane_reference(own_faces, face_source, send_rows):
    devices = send_rows.shape[0]
    table = own_faces[:, :4].reshape((devices, -1) + own_faces.shape[2:])
    buffers = jax.vmap(send_buffers)(table, send_rows[:, None])
    received = jnp.stack([jnp.roll(buffers[:, 1], 1, axis=0), buffers[:, 0], buffers[:, 1], jnp.roll(buffers[:, 0], -1, axis=0)], axis=1)
    plane = jax.vmap(pick_outside)(table, received, face_source.reshape(devices, -1, 4))
    plane = plane.reshape((-1,) + plane.shape[2:])
    return [plane[:, 0], plane[:, 1], plane[:, 2], plane[:, 3]]

def reference(state, direction, metric, face_source, send_rows):
    element = (5, 5, 5, 5)
    primal = jnp.moveaxis(state.reshape((PLANE, LAYERS) + element), 1, 0)[:, :, None]
    tangent = jnp.moveaxis(direction.reshape((PLANE, LAYERS) + element), 1, 0)[:, :, None]
    scales = jnp.moveaxis(metric, 1, 0)[:, :, None]
    walls = wall_masks(face_source)
    lead_shape = (LAYERS, PLANE, 1, -1)
    bottoms = jnp.concatenate([face_slice(primal, 4).reshape(lead_shape), face_slice(tangent, 4).reshape(lead_shape)], axis=-1)
    tops = jnp.concatenate([face_slice(primal, 5).reshape(lead_shape), face_slice(tangent, 5).reshape(lead_shape)], axis=-1)
    below_states = jnp.roll(tops, 1, axis=0)
    above_states = jnp.roll(bottoms, -1, axis=0)

    def first_section(volume_p, volume_t, scales_layer, below, above):
        own_states = jnp.concatenate([pack_faces(volume_p), pack_faces(volume_t)], axis=-1)
        outside = plane_reference(own_states, face_source, send_rows) + [below, above]
        outside_p = with_walls(split_traces(outside, 0, (5, 5, 5)), volume_p, walls)
        outside_t = with_walls(split_traces(outside, 1, (5, 5, 5)), volume_t, walls)
        grad_p, grad_t = jax.jvp(lambda volume, outer_side: lifted_gradient(volume, outer_side, scales_layer), (volume_p, outside_p), (volume_t, outside_t))
        return (outside_p, outside_t, grad_p, grad_t)

    def visc_section(inputs):
        volume_p, volume_t, scales_layer, below, above = inputs
        outside_p, outside_t, grad_p, grad_t = first_section(volume_p, volume_t, scales_layer, below, above)
        visc_p, visc_t = jax.jvp(own_viscous_faces, (volume_p, grad_p), (volume_t, grad_t))
        return jnp.concatenate([stack_faces(visc_p), stack_faces(visc_t)], axis=-1)
    own_visc = lax.map(visc_section, (primal, tangent, scales, below_states, above_states))
    visc_below = jnp.roll(own_visc[:, :, 5], 1, axis=0)
    visc_above = jnp.roll(own_visc[:, :, 4], -1, axis=0)

    def final_section(inputs):
        volume_p, volume_t, scales_layer, below, above, visc_own, visc_low, visc_high = inputs
        outside_p, outside_t, grad_p, grad_t = first_section(volume_p, volume_t, scales_layer, below, above)
        visc_out = plane_reference(visc_own, face_source, send_rows) + [visc_low, visc_high]
        visc_p = split_traces(visc_out, 0, (5, 5, 5))
        visc_t = split_traces(visc_out, 1, (5, 5, 5))
        return jax.jvp(lambda volume, outer_side, gradients, visc_side: residual_terms(volume, outer_side, gradients, visc_side, scales_layer, walls), (volume_p, outside_p, grad_p, visc_p), (volume_t, outside_t, grad_t, visc_t))
    res_p, res_t = lax.map(final_section, (primal, tangent, scales, below_states, above_states, own_visc, visc_below, visc_above))
    residual = jnp.moveaxis(res_p[:, :, 0], 0, 1).reshape(state.shape)
    product = jnp.moveaxis(res_t[:, :, 0], 0, 1).reshape(state.shape)
    total = float(state.size)
    coefficient = jnp.sum(direction * product) / total
    remainder = product - coefficient * direction
    beta = jnp.sqrt(jnp.sum(remainder * remainder) / total)
    norm_value = jnp.sqrt(jnp.sum(residual * residual) / total)
    return (residual, remainder / beta, jnp.stack([coefficient, beta, norm_value]))
```

```python
import functools
import math

import jax
import jax.numpy as jnp
import numpy as np
from jax import lax
from jax.experimental import pallas as pl
from jax.experimental.pallas import tpu as pltpu
from jax.sharding import PartitionSpec as P

GAMMA = 1.4
VISC = 0.01
COND = VISC * GAMMA / ((GAMMA - 1.0) * 0.72)
LIFT = 10.0
MESH = pl.DeviceIdType.MESH
F32, BF16 = jnp.float32, jnp.bfloat16


def diff_table():
    spread = math.sqrt(3.0 / 7.0)
    points = np.array([-1.0, -spread, 0.0, spread, 1.0])
    weights = np.array(
        [np.prod([points[i] - points[j] for j in range(5) if j != i]) for i in range(5)]
    )
    matrix = np.zeros((5, 5))
    for i in range(5):
        for j in range(5):
            if i != j:
                matrix[i, j] = weights[i] / (weights[j] * (points[i] - points[j]))
        matrix[i, i] = np.sum([1.0 / (points[i] - points[j]) for j in range(5) if j != i])
    return matrix


def operators(layers):
    table = diff_table()
    eye = np.eye(5)
    kron = [
        np.einsum("ai,bj,ck->ijkabc", *[table if m == a else eye for m in range(3)]).reshape(125, 125)
        for a in range(3)
    ]
    node = np.arange(125).reshape(5, 5, 5)
    vw, fw, half = 128 * layers, 64 * layers, 32 * layers
    deriv = np.zeros((3, vw, vw), np.float32)
    pick = np.zeros((3, vw, fw), np.float32)
    for a in range(3):
        for l in range(layers):
            b = 128 * l
            deriv[a, b : b + 125, b : b + 125] = kron[a]
            for side in range(2):
                face = np.take(node, 4 * side, axis=a).reshape(-1)
                for m, at in enumerate(face):
                    pick[a, b + at, side * half + 32 * l + m] = 1.0
    high = deriv.astype(jnp.bfloat16)
    low = (deriv - high.astype(np.float32)).astype(jnp.bfloat16)
    lift = np.swapaxes(pick, 1, 2)
    return high, low, pick.astype(jnp.bfloat16), lift.astype(jnp.bfloat16)


def pieces(x, n):
    out = []
    for i in range(n):
        p = x.astype(BF16)
        out.append(p)
        if i + 1 < n:
            x = x - p.astype(F32)
    return out


def dot(a, b):
    return jnp.dot(a, b, preferred_element_type=F32)


def left(x, w, n):
    return sum(dot(p, w) for p in pieces(x, n)[::-1])


def right(w, x, n):
    return sum(dot(w, p) for p in pieces(x, n)[::-1])


def derive(x, high, low):
    a, b = pieces(x, 2)
    return dot(a, low) + dot(b, high) + dot(a, high)


def fields_of(u):
    inv = 1.0 / u[0]
    vel = [u[1] * inv, u[2] * inv, u[3] * inv]
    kinetic = 0.5 * (u[1] * vel[0] + u[2] * vel[1] + u[3] * vel[2])
    pressure = (GAMMA - 1.0) * (u[4] - kinetic)
    return vel, pressure, pressure * inv


def inviscid(u, a):
    vel, pressure, _ = fields_of(u)
    out = [u[1 + a]]
    for m in range(3):
        term = u[1 + m] * vel[a]
        out.append(term + pressure if m == a else term)
    out.append((u[4] + pressure) * vel[a])
    return out


def viscous(vel, q, a, divergence):
    stress = []
    for m in range(3):
        term = q[a][m] + q[m][a]
        if m == a:
            term = term - 2.0 / 3.0 * divergence
        stress.append(VISC * term)
    energy = stress[0] * vel[0] + stress[1] * vel[1] + stress[2] * vel[2] + COND * q[a][3]
    return stress + [energy]


def viscous_all(u, q):
    inv = 1.0 / u[0]
    vel = [u[1] * inv, u[2] * inv, u[3] * inv]
    divergence = q[0][0] + q[1][1] + q[2][2]
    return [viscous(vel, q, a, divergence) for a in range(3)]


def gradient_fields(u):
    vel, _, temper = fields_of(u)
    return vel + [temper]


def jump_fields(inner, outer):
    return [o - i for o, i in zip(gradient_fields(outer), gradient_fields(inner))]


def surface(inner, outer, sign, a):
    vi, pi, ti = fields_of(inner)
    vo, po, to = fields_of(outer)
    square = sum(v * v for v in vi) + GAMMA * ti + sum(v * v for v in vo) + GAMMA * to
    speed = jnp.sqrt(0.5 * square)
    fi, fo = inviscid(inner, a), inviscid(outer, a)
    return [
        (0.5 * LIFT) * (sign * (fo[m] - fi[m]) - speed * (outer[m] - inner[m])) for m in range(5)
    ]


def kernel(
    ns, np_, total_count,
    x_ref, d_ref, metric_ref, fs_ref, sr_ref, keyrow_ref, dh_ref, dl_ref, pick_ref, lift_ref,
    res_ref, basis_ref, kry_ref,
    u, uf, of, w, jf, q, v, vf, ov, g, s, r, mv, mf,
    sb1, rb1, zs1, zr1, sb2, rb2, zs2, zr2, st, sta, stb,
    xsend, xrecv, asend, arecv, bsend, brecv,
):
    C, L = x_ref.shape[0], x_ref.shape[1]
    VW, FW, half = 128 * L, 64 * L, 32 * L
    SLOTS = sr_ref.shape[2]
    SP = sb1.shape[1]
    OWN = 4 * C
    ms, mp = lax.axis_index("stream"), lax.axis_index("span")
    lower, upper = lax.rem(ms + ns - 1, ns), lax.rem(ms + 1, ns)
    below, above = lax.rem(mp + np_ - 1, np_), lax.rem(mp + 1, np_)

    barrier = pltpu.get_barrier_semaphore()
    for k in range(1, ns):
        pl.semaphore_signal(
            barrier, inc=1, device_id=(lax.rem(ms + k, ns), mp), device_id_type=MESH
        )
    for k in range(1, np_):
        pl.semaphore_signal(
            barrier, inc=1, device_id=(ms, lax.rem(mp + k, np_)), device_id_type=MESH
        )

    fl = lax.broadcasted_iota(jnp.int32, (1, FW), 1)
    vl = lax.broadcasted_iota(jnp.int32, (1, VW), 1)
    first = fl < half
    sign = jnp.where(first, -1.0, 1.0)
    flayer = lax.rem(fl, half) // 32
    fpad = jnp.where(lax.rem(fl, 32) >= 25, 1.0, 0.0)

    for pt, ref in enumerate((x_ref, d_ref)):
        for l in range(L):
            for m in range(5):
                pad = 1.0 if pt == 0 and m % 4 == 0 else 0.0
                u[pt, m, :, 128 * l + 120 : 128 * (l + 1)] = jnp.full((C, 8), pad, F32)
                u[pt, m, :, 128 * l : 128 * l + 125] = ref[:, l, 125 * m : 125 * (m + 1)]
    for a in range(3):
        wide = jnp.zeros((C, VW), F32)
        face = jnp.zeros((C, FW), F32)
        for l in range(L):
            value = metric_ref[:, l, a : a + 1]
            wide = jnp.where(vl // 128 == l, value, wide)
            face = jnp.where(flayer == l, value, face)
        mv[a] = wide
        mf[a] = face

    keyrow = keyrow_ref[...]
    onehot = jnp.concatenate(
        [
            jnp.where(fs_ref[:, 2 * a + side : 2 * a + side + 1] == keyrow, 1.0, 0.0)
            for side in range(2)
            for a in range(2)
        ],
        axis=0,
    ).astype(BF16)
    hot_own, hot_recv = onehot[:, :OWN], onehot[:, OWN : OWN + 2 * SP]
    ri = lax.broadcasted_iota(jnp.int32, (SP, SLOTS), 0)
    li = lax.broadcasted_iota(jnp.int32, (SP, SLOTS), 1)
    send_hot = []
    for side in range(2):
        row = sr_ref[0, side : side + 1, :].astype(F32)
        column = jnp.sum(jnp.where(ri == li, row, 0.0), axis=1, keepdims=True)
        send_hot.append(jnp.where(column == keyrow[:, :OWN].astype(F32), 1.0, 0.0))
    send_hot = jnp.concatenate(send_hot, axis=0).astype(BF16)

    def swap(a, b):
        return (
            jnp.where(first, a, pltpu.roll(b, half, 1)),
            jnp.where(first, pltpu.roll(a, half, 1), b),
        )

    def exchange(faces, members, sb, rb, zs, zr, base):
        blocks = [[swap(faces(0, m, a), faces(1, m, a)) for m in range(members)] for a in range(3)]
        table = jnp.concatenate(
            [
                jnp.concatenate([blocks[a][m][side] for m in range(members)], axis=1)
                for side in range(2)
                for a in range(2)
            ],
            axis=0,
        )
        for side in range(2):
            for m in range(members):
                zs[side, :, FW * m : FW * (m + 1)] = blocks[2][m][side]
        zs_copies = [
            (zs.at[0], zr.at[1], (ms, below)),
            (zs.at[1], zr.at[0], (ms, above)),
        ]
        copies = []
        for i, (src, dst, to) in enumerate(zs_copies):
            copies.append(
                pltpu.make_async_remote_copy(
                    src_ref=src, dst_ref=dst, send_sem=xsend.at[base + i],
                    recv_sem=xrecv.at[base + i], device_id=to, device_id_type=MESH,
                )
            )
        table_pieces = pieces(table, 3)
        sent = sum(dot(send_hot, p) for p in table_pieces[::-1])
        return blocks, table_pieces, sent, copies

    def finish_send(sent, sb, rb, base):
        sb[0] = sent[:SP]
        sb[1] = sent[SP:]
        out = []
        for i, (src, dst, to) in enumerate(
            [(sb.at[0], rb.at[1], (lower, mp)), (sb.at[1], rb.at[0], (upper, mp))]
        ):
            out.append(
                pltpu.make_async_remote_copy(
                    src_ref=src, dst_ref=dst, send_sem=xsend.at[base + 2 + i],
                    recv_sem=xrecv.at[base + 2 + i], device_id=to, device_id_type=MESH,
                )
            )
        return out

    def plane_outside(own, rb, members, put):
        received = jnp.concatenate([rb[0], rb[1]], axis=0)
        got = own + right(hot_recv, received, 3)
        for a in range(2):
            for m in range(members):
                lanes = slice(FW * m, FW * (m + 1))
                lo = got[a * C : (a + 1) * C, lanes]
                hi = got[(2 + a) * C : (3 + a) * C, lanes]
                primal, tangent = swap(lo, hi)
                put(0, m, a, primal)
                put(1, m, a, tangent)

    def layer_outside(blocks, zr, members, put):
        step = (L - 1) * 32
        for m in range(members):
            lanes = slice(FW * m, FW * (m + 1))
            lo = jnp.where(
                flayer == 0,
                pltpu.roll(zr[0, :, lanes], (FW - step) % FW, 1),
                pltpu.roll(blocks[2][m][1], 32, 1),
            )
            hi = jnp.where(
                flayer == L - 1,
                pltpu.roll(zr[1, :, lanes], step, 1),
                pltpu.roll(blocks[2][m][0], FW - 32, 1),
            )
            primal, tangent = swap(lo, hi)
            put(0, m, 2, primal)
            put(1, m, 2, tangent)

    whole = u[...].reshape(10 * C, VW)
    for a in range(3):
        faces = left(whole, pick_ref[a], 3).reshape(2, 5, C, FW)
        for m in range(5):
            uf[0, m, a] = faces[0, m] + fpad if m % 4 == 0 else faces[0, m]
            uf[1, m, a] = faces[1, m]
    blocks1, table1, sent1, zcopies1 = exchange(
        lambda pt, m, a: uf[pt, m, a], 5, sb1, rb1, zs1, zr1, 0
    )
    pl.semaphore_wait(barrier, ns + np_ - 2)
    for copy in zcopies1:
        copy.start()
    pcopies1 = finish_send(sent1, sb1, rb1, 0)
    for copy in pcopies1:
        copy.start()

    own1 = sum(dot(hot_own, p) for p in table1[::-1])

    @pl.loop(0, C // 8)
    def _(i):
        rows = pl.ds(pl.multiple_of(i * 8, 8), 8)
        primal = [u[0, m, rows, :] for m in range(5)]
        tangent = [u[1, m, rows, :] for m in range(5)]
        fp, ft = jax.jvp(gradient_fields, (primal,), (tangent,))
        for m in range(4):
            w[0, m, rows, :] = fp[m]
            w[1, m, rows, :] = ft[m]

    fields = w[...].reshape(8 * C, VW)
    for a in range(3):
        q[a] = derive(fields, dh_ref[a], dl_ref[a]).reshape(2, 4, C, VW)

    for copy in zcopies1 + pcopies1:
        copy.wait()
    low_wall = jnp.where(fs_ref[:, 2:3] < 0, 1.0, 0.0)
    high_wall = jnp.where(fs_ref[:, 3:4] < 0, 1.0, 0.0)
    wall = jnp.where(first, low_wall, high_wall) > 0.5

    def put1(pt, m, a, value):
        if a == 1:
            own = uf[pt, m, a]
            value = jnp.where(wall, own if m % 4 == 0 else -own, value)
        of[pt, m, a] = value

    plane_outside(own1, rb1, 5, put1)
    layer_outside(blocks1, zr1, 5, put1)

    for a in range(3):
        @pl.loop(0, C // 8)
        def _(i):
            rows = pl.ds(pl.multiple_of(i * 8, 8), 8)
            primal = ([uf[0, m, a, rows, :] for m in range(5)], [of[0, m, a, rows, :] for m in range(5)])
            tangent = ([uf[1, m, a, rows, :] for m in range(5)], [of[1, m, a, rows, :] for m in range(5)])
            jp, jt = jax.jvp(jump_fields, primal, tangent)
            for m in range(4):
                jf[a, 0, m, rows, :] = (0.5 * LIFT) * sign * jp[m]
                jf[a, 1, m, rows, :] = (0.5 * LIFT) * sign * jt[m]

        q[a] += left(jf[a].reshape(8 * C, FW), lift_ref[a], 2).reshape(2, 4, C, VW)

    @pl.loop(0, C // 8)
    def _(i):
        rows = pl.ds(pl.multiple_of(i * 8, 8), 8)
        scale = [mv[a, rows, :] for a in range(3)]
        states = [[u[pt, m, rows, :] for m in range(5)] for pt in range(2)]
        grads = [
            [[scale[a] * q[a, pt, m, rows, :] for m in range(4)] for a in range(3)]
            for pt in range(2)
        ]
        vp, vt = jax.jvp(viscous_all, (states[0], grads[0]), (states[1], grads[1]))
        for a in range(3):
            for m in range(4):
                v[a, 0, m, rows, :] = vp[a][m]
                v[a, 1, m, rows, :] = vt[a][m]

    for a in range(3):
        vf[a] = left(v[a].reshape(8 * C, VW), pick_ref[a], 3).reshape(2, 4, C, FW)
    blocks2, table2, sent2, zcopies2 = exchange(
        lambda pt, m, a: vf[a, pt, m], 4, sb2, rb2, zs2, zr2, 4
    )
    for copy in zcopies2:
        copy.start()
    pcopies2 = finish_send(sent2, sb2, rb2, 4)
    for copy in pcopies2:
        copy.start()

    own2 = sum(dot(hot_own, p) for p in table2[::-1])

    @pl.loop(0, C // 8)
    def _(i):
        rows = pl.ds(pl.multiple_of(i * 8, 8), 8)
        states = [[u[pt, m, rows, :] for m in range(5)] for pt in range(2)]
        for a in range(3):
            scale = mv[a, rows, :]
            fluxes = jax.jvp(lambda x: inviscid(x, a), (states[0],), (states[1],))
            for pt in range(2):
                g[a, pt, 0, rows, :] = scale * fluxes[pt][0]
                for m in range(4):
                    g[a, pt, m + 1, rows, :] = scale * (fluxes[pt][m + 1] - v[a, pt, m, rows, :])

    for a in range(3):
        @pl.loop(0, C // 8)
        def _(i):
            rows = pl.ds(pl.multiple_of(i * 8, 8), 8)
            primal = ([uf[0, m, a, rows, :] for m in range(5)], [of[0, m, a, rows, :] for m in range(5)])
            tangent = ([uf[1, m, a, rows, :] for m in range(5)], [of[1, m, a, rows, :] for m in range(5)])
            sp, stt = jax.jvp(
                lambda inner, outer: surface(inner, outer, sign, a), primal, tangent
            )
            for m in range(5):
                s[a, 0, m, rows, :] = sp[m]
                s[a, 1, m, rows, :] = stt[m]

    total = None
    for a in range(3):
        part = derive(g[a].reshape(10 * C, VW), dh_ref[a], dl_ref[a])
        total = part if total is None else total + part
    r[...] = total.reshape(2, 5, C, VW)

    for copy in zcopies2 + pcopies2:
        copy.wait()

    def put2(pt, m, a, value):
        if a == 1:
            value = jnp.where(wall, vf[a, pt, m], value)
        ov[a, pt, m] = value

    plane_outside(own2, rb2, 4, put2)
    layer_outside(blocks2, zr2, 4, put2)
    lifted = None
    for a in range(3):
        for pt in range(2):
            s[a, pt, 0] = mf[a] * s[a, pt, 0]
            for m in range(4):
                jump = ov[a, pt, m] - vf[a, pt, m]
                s[a, pt, m + 1] = mf[a] * (s[a, pt, m + 1] - (0.5 * LIFT) * sign * jump)
        part = left(s[a].reshape(10 * C, FW), lift_ref[a], 2)
        lifted = part if lifted is None else lifted + part
    r[...] += lifted.reshape(2, 5, C, VW)

    def whole_sum(parts):
        acc = parts[0]
        for part in parts[1:]:
            acc = acc + part
        return jnp.sum(jnp.sum(acc, axis=0, keepdims=True), axis=1, keepdims=True)

    def ratio(top, bottom):
        return jnp.where(bottom > 0.0, top / jnp.where(bottom > 0.0, bottom, 1.0), 0.0)

    pd = whole_sum([r[1, m] * u[1, m] for m in range(5)])
    dd = whole_sum([u[1, m] * u[1, m] for m in range(5)])
    rs = whole_sum([r[0, m] * r[0, m] for m in range(5)])
    mine = ratio(pd, dd)
    rests = [r[1, m] - mine * u[1, m] for m in range(5)]
    rr = whole_sum([x * x for x in rests])
    rd = whole_sum([x * u[1, m] for m, x in enumerate(rests)])
    stats = [jnp.broadcast_to(x, (1, 128)) for x in (pd, dd, rs, rr, rd)]

    def write(stats):
        for i in range(5):
            st[i : i + 1, :] = stats[i]
        st[5:8, :] = jnp.zeros((3, 128), F32)

    def gathered(n, buf, ssem, rsem, peer):
        copies = []
        for k in range(1, n):
            copy = pltpu.make_async_remote_copy(
                src_ref=st, dst_ref=buf.at[k], send_sem=ssem.at[k], recv_sem=rsem.at[k],
                device_id=peer(k), device_id_type=MESH,
            )
            copy.start()
            copies.append(copy)
        buf[0] = st[...]
        for copy in copies:
            copy.wait()
        pd, dd, rs, rr, rd = [buf[:, i, :] for i in range(5)]
        own = ratio(pd, dd)
        add = lambda x: jnp.sum(x, axis=0, keepdims=True)
        pd0, dd0 = add(pd), add(dd)
        shift = own - ratio(pd0, dd0)
        rr0 = add(rr + 2.0 * shift * rd + shift * shift * dd)
        return [pd0, dd0, add(rs), rr0, add(rd + shift * dd)]

    write(stats)
    stats = gathered(np_, sta, asend, arecv, lambda k: (ms, lax.rem(mp + k, np_)))
    for l in range(L):
        for m in range(5):
            res_ref[:, l, 125 * m : 125 * (m + 1)] = r[0, m, :, 128 * l : 128 * l + 125]
    write(stats)
    pd, dd, rs, rr, rd = gathered(ns, stb, bsend, brecv, lambda k: (lax.rem(ms + k, ns), mp))
    coefficient = pd * (1.0 / total_count)
    shift = ratio(pd, dd) - coefficient
    beta = jnp.sqrt((rr + 2.0 * shift * rd + shift * shift * dd) * (1.0 / total_count))
    norm = jnp.sqrt(rs * (1.0 / total_count))
    lane = lax.broadcasted_iota(jnp.int32, (1, 128), 1)
    kry_ref[...] = jnp.where(lane == 0, coefficient, jnp.where(lane == 1, beta, norm))
    c, inv = coefficient[:, :1], 1.0 / beta[:, :1]
    for m in range(5):
        value = (r[1, m] - c * u[1, m]) * inv
        for l in range(L):
            basis_ref[:, l, 125 * m : 125 * (m + 1)] = value[:, 128 * l : 128 * l + 125]


def local(ns, np_, state, direction, metric, face_source, send_rows):
    C, L, width = state.shape
    slots = send_rows.shape[2]
    SP = -(-slots // 8) * 8
    VW, FW = 128 * L, 64 * L
    own = 4 * C
    keys = np.full((1, own + 2 * SP), -7, np.int32)
    side, rest = np.divmod(np.arange(own), 2 * C)
    keys[0, :own] = 4 * (rest % C) + 2 * (rest // C) + side
    keys[0, own : own + slots] = own + np.arange(slots)
    keys[0, own + SP : own + SP + slots] = own + slots + np.arange(slots)
    high, low, pick, lift = operators(L)
    vmem = lambda *shape: pltpu.VMEM(shape, F32)
    dma = lambda n: pltpu.SemaphoreType.DMA((n,))
    spec = pl.BlockSpec(memory_space=pltpu.VMEM)
    residual, basis, krylov = pl.pallas_call(
        functools.partial(kernel, ns, np_, float(state.size * ns * np_)),
        out_shape=(
            jax.ShapeDtypeStruct(state.shape, F32),
            jax.ShapeDtypeStruct(state.shape, F32),
            jax.ShapeDtypeStruct((1, 128), F32),
        ),
        in_specs=[spec] * 10,
        out_specs=(spec,) * 3,
        scratch_shapes=[
            vmem(2, 5, C, VW), vmem(2, 5, 3, C, FW), vmem(2, 5, 3, C, FW),
            vmem(2, 4, C, VW), vmem(3, 2, 4, C, FW), vmem(3, 2, 4, C, VW),
            vmem(3, 2, 4, C, VW), vmem(3, 2, 4, C, FW), vmem(3, 2, 4, C, FW),
            vmem(3, 2, 5, C, VW), vmem(3, 2, 5, C, FW), vmem(2, 5, C, VW),
            vmem(3, C, VW), vmem(3, C, FW),
            vmem(2, SP, 5 * FW), vmem(2, SP, 5 * FW), vmem(2, C, 5 * FW), vmem(2, C, 5 * FW),
            vmem(2, SP, 4 * FW), vmem(2, SP, 4 * FW), vmem(2, C, 4 * FW), vmem(2, C, 4 * FW),
            vmem(8, 128), vmem(np_, 8, 128), vmem(ns, 8, 128),
            dma(8), dma(8), dma(np_), dma(np_), dma(ns), dma(ns),
        ],
        compiler_params=pltpu.CompilerParams(
            collective_id=0, has_side_effects=True, vmem_limit_bytes=48 * 1024 * 1024
        ),
        name="navier",
    )(
        state, direction, metric, face_source, send_rows,
        jnp.asarray(keys), jnp.asarray(high), jnp.asarray(low), jnp.asarray(pick), jnp.asarray(lift),
    )
    return residual, basis, krylov[0, :3]


def solution(mesh):
    return jax.shard_map(
        functools.partial(local, mesh.shape["stream"], mesh.shape["span"]),
        mesh=mesh,
        in_specs=(
            P("stream", "span", None),
            P("stream", "span", None),
            P("stream", "span", None),
            P("stream", None),
            P("stream", None, None),
        ),
        out_specs=(P("stream", "span", None), P("stream", "span", None), P()),
        check_vma=False,
    )
```

```python
import functools
import math

import jax
import jax.numpy as jnp
import numpy as np
from jax import lax
from jax.experimental import pallas as pl
from jax.experimental.pallas import tpu as pltpu
from jax.sharding import PartitionSpec as P

GAMMA = 1.4
VISC = 0.01
COND = VISC * GAMMA / ((GAMMA - 1.0) * 0.72)
LIFT = 10.0
MESH = pl.DeviceIdType.MESH
F32, BF16 = jnp.float32, jnp.bfloat16


def diff_table():
    spread = math.sqrt(3.0 / 7.0)
    points = np.array([-1.0, -spread, 0.0, spread, 1.0])
    weights = np.array(
        [np.prod([points[i] - points[j] for j in range(5) if j != i]) for i in range(5)]
    )
    matrix = np.zeros((5, 5))
    for i in range(5):
        for j in range(5):
            if i != j:
                matrix[i, j] = weights[i] / (weights[j] * (points[i] - points[j]))
        matrix[i, i] = np.sum([1.0 / (points[i] - points[j]) for j in range(5) if j != i])
    return matrix


def operators(layers):
    table = diff_table()
    eye = np.eye(5)
    kron = [
        np.einsum("ai,bj,ck->ijkabc", *[table if m == a else eye for m in range(3)]).reshape(125, 125)
        for a in range(3)
    ]
    node = np.arange(125).reshape(5, 5, 5)
    vw, fw, half = 128 * layers, 64 * layers, 32 * layers
    deriv = np.zeros((3, vw, vw), np.float32)
    pick = np.zeros((3, vw, fw), np.float32)
    for a in range(3):
        for l in range(layers):
            b = 128 * l
            deriv[a, b : b + 125, b : b + 125] = kron[a]
            for side in range(2):
                face = np.take(node, 4 * side, axis=a).reshape(-1)
                for m, at in enumerate(face):
                    pick[a, b + at, side * half + 32 * l + m] = 1.0
    high = deriv.astype(jnp.bfloat16)
    low = (deriv - high.astype(np.float32)).astype(jnp.bfloat16)
    lift = np.swapaxes(pick, 1, 2)
    return high, low, pick.astype(jnp.bfloat16), lift.astype(jnp.bfloat16)


def pieces(x, n):
    out = []
    for i in range(n):
        p = x.astype(BF16)
        out.append(p)
        if i + 1 < n:
            x = x - p.astype(F32)
    return out


def dot(a, b):
    return jnp.dot(a, b, preferred_element_type=F32)


def left(x, w, n):
    return sum(dot(p, w) for p in pieces(x, n)[::-1])


def right(w, x, n):
    return sum(dot(w, p) for p in pieces(x, n)[::-1])


def derive(x, high, low):
    a, b = pieces(x, 2)
    return dot(a, low) + dot(b, high) + dot(a, high)


def fields_of(u):
    inv = 1.0 / u[0]
    vel = [u[1] * inv, u[2] * inv, u[3] * inv]
    kinetic = 0.5 * (u[1] * vel[0] + u[2] * vel[1] + u[3] * vel[2])
    pressure = (GAMMA - 1.0) * (u[4] - kinetic)
    return vel, pressure, pressure * inv


def inviscid(u, a):
    vel, pressure, _ = fields_of(u)
    out = [u[1 + a]]
    for m in range(3):
        term = u[1 + m] * vel[a]
        out.append(term + pressure if m == a else term)
    out.append((u[4] + pressure) * vel[a])
    return out


def viscous(vel, q, a, divergence):
    stress = []
    for m in range(3):
        term = q[a][m] + q[m][a]
        if m == a:
            term = term - 2.0 / 3.0 * divergence
        stress.append(VISC * term)
    energy = stress[0] * vel[0] + stress[1] * vel[1] + stress[2] * vel[2] + COND * q[a][3]
    return stress + [energy]


def viscous_all(u, q):
    inv = 1.0 / u[0]
    vel = [u[1] * inv, u[2] * inv, u[3] * inv]
    divergence = q[0][0] + q[1][1] + q[2][2]
    return [viscous(vel, q, a, divergence) for a in range(3)]


def gradient_fields(u):
    vel, _, temper = fields_of(u)
    return vel + [temper]


def jump_fields(inner, outer):
    return [o - i for o, i in zip(gradient_fields(outer), gradient_fields(inner))]


def surface(inner, outer, sign, a):
    vi, pi, ti = fields_of(inner)
    vo, po, to = fields_of(outer)
    square = sum(v * v for v in vi) + GAMMA * ti + sum(v * v for v in vo) + GAMMA * to
    speed = jnp.sqrt(0.5 * square)
    fi, fo = inviscid(inner, a), inviscid(outer, a)
    return [
        (0.5 * LIFT) * (sign * (fo[m] - fi[m]) - speed * (outer[m] - inner[m])) for m in range(5)
    ]


def kernel(
    ns, np_, total_count,
    x_hbm, d_hbm, metric_hbm, fs_hbm, sr_hbm, key_hbm, dh_hbm, dl_hbm, pick_hbm, lift_hbm,
    res_ref, basis_ref, kry_ref,
    u, uf, of, w, jf, q, v, vf, ov, g, s, r, mv, mf,
    sb1, rb1, zs1, zr1, sb2, rb2, zs2, zr2, st, sta,
    x_ref, d_ref, metric_ref, fs_ref, sr_ref, keyrow_ref, dh_ref, dl_ref, pick_ref, lift_ref,
    xsend, xrecv, asend, arecv, loads,
):
    C, L = x_ref.shape[0], x_ref.shape[1]
    VW, FW, half = 128 * L, 64 * L, 32 * L
    SLOTS = sr_ref.shape[2]
    SP = sb1.shape[1]
    OWN = 4 * C
    ms, mp = lax.axis_index("stream"), lax.axis_index("span")
    lower, upper = lax.rem(ms + ns - 1, ns), lax.rem(ms + 1, ns)
    below, above = lax.rem(mp + np_ - 1, np_), lax.rem(mp + 1, np_)

    inputs = [
        pltpu.make_async_copy(src, dst, loads.at[i])
        for i, (src, dst) in enumerate(
            [
                (x_hbm, x_ref), (d_hbm, d_ref), (pick_hbm, pick_ref), (key_hbm, keyrow_ref),
                (fs_hbm, fs_ref), (sr_hbm, sr_ref), (metric_hbm, metric_ref),
                (dh_hbm, dh_ref), (dl_hbm, dl_ref), (lift_hbm, lift_ref),
            ]
        )
    ]
    for copy in inputs:
        copy.start()

    def peer(k):
        a, b = divmod(k, np_)
        return lax.rem(ms + a, ns), lax.rem(mp + b, np_)

    everyone = ns * np_
    barrier = pltpu.get_barrier_semaphore()
    for k in range(1, everyone):
        pl.semaphore_signal(barrier, inc=1, device_id=peer(k), device_id_type=MESH)

    fl = lax.broadcasted_iota(jnp.int32, (1, FW), 1)
    vl = lax.broadcasted_iota(jnp.int32, (1, VW), 1)
    first = fl < half
    sign = jnp.where(first, -1.0, 1.0)
    flayer = lax.rem(fl, half) // 32
    fnode = lax.rem(fl, 32)
    fpad = jnp.where(fnode >= 25, 1.0, 0.0)

    def roll(x, shift):
        shift = shift % FW
        return pltpu.roll(x, shift, 1) if shift else x

    di = lax.broadcasted_iota(jnp.int32, (C, C), 0)
    dj = lax.broadcasted_iota(jnp.int32, (C, C), 1)

    def column(row):
        return jnp.sum(jnp.where(di == dj, row, 0.0), axis=1, keepdims=True)

    for copy in inputs[:2]:
        copy.wait()

    for pt, ref in enumerate((x_ref, d_ref)):
        for l in range(L):
            for m in range(5):
                pad = 1.0 if pt == 0 and m % 4 == 0 else 0.0
                u[pt, m, :, 128 * l + 120 : 128 * (l + 1)] = jnp.full((C, 8), pad, F32)
                u[pt, m, :, 128 * l : 128 * l + 125] = ref[:, l, 125 * m : 125 * (m + 1)]
    for copy in inputs[2:7]:
        copy.wait()
    keyrow = keyrow_ref[...].astype(F32)
    source = [column(fs_ref[f : f + 1, :].astype(F32)) for f in range(4)]
    onehot = jnp.concatenate(
        [
            jnp.where(source[2 * a + side] == keyrow, 1.0, 0.0)
            for side in range(2)
            for a in range(2)
        ],
        axis=0,
    ).astype(BF16)
    hot_own, hot_recv = onehot[:, :OWN], onehot[:, OWN : OWN + 2 * SP]
    ri = lax.broadcasted_iota(jnp.int32, (SP, SLOTS), 0)
    li = lax.broadcasted_iota(jnp.int32, (SP, SLOTS), 1)
    send_hot = []
    for side in range(2):
        row = sr_ref[0, side : side + 1, :].astype(F32)
        wanted = jnp.sum(jnp.where(ri == li, row, 0.0), axis=1, keepdims=True)
        send_hot.append(jnp.where(wanted == keyrow[:, :OWN], 1.0, 0.0))
    send_hot = jnp.concatenate(send_hot, axis=0).astype(BF16)

    def swap(a, b):
        return (
            jnp.where(first, a, pltpu.roll(b, half, 1)),
            jnp.where(first, pltpu.roll(a, half, 1), b),
        )

    def exchange(faces, members, sb, rb, zs, zr, base):
        blocks = [[swap(faces(0, m, a), faces(1, m, a)) for m in range(members)] for a in range(3)]
        table = jnp.concatenate(
            [
                jnp.concatenate([blocks[a][m][side] for m in range(members)], axis=1)
                for side in range(2)
                for a in range(2)
            ],
            axis=0,
        )
        for m in range(0, members, 2):
            for side in range(2):
                value = blocks[2][m][side]
                if m + 1 < members:
                    other = roll(blocks[2][m + 1][side], 32 if side == 0 else -32)
                    value = jnp.where(flayer == (0 if side == 0 else L - 1), value, other)
                zs[side, :, FW * (m // 2) : FW * (m // 2 + 1)] = value
        zs_copies = [
            (zs.at[0], zr.at[1], (ms, below)),
            (zs.at[1], zr.at[0], (ms, above)),
        ]
        copies = []
        for i, (src, dst, to) in enumerate(zs_copies):
            copies.append(
                pltpu.make_async_remote_copy(
                    src_ref=src, dst_ref=dst, send_sem=xsend.at[base + i],
                    recv_sem=xrecv.at[base + i], device_id=to, device_id_type=MESH,
                )
            )
        table_pieces = pieces(table, 3)
        sent = sum(dot(send_hot, p) for p in table_pieces[::-1])
        return blocks, table_pieces, sent, copies

    def finish_send(sent, sb, rb, base):
        width = sb.shape[2]
        for m in range(width // FW):
            value = sent[:, FW * m : FW * (m + 1)]
            if sent.shape[1] > width:
                spare = roll(sent[:, width:], 25 - 7 * m)
                value = jnp.where(fnode < 25, value, spare)
            sb[0, :, FW * m : FW * (m + 1)] = value[:SP]
            sb[1, :, FW * m : FW * (m + 1)] = value[SP:]
        out = []
        for i, (src, dst, to) in enumerate(
            [
                (sb.at[0], rb.at[1], (lower, mp)),
                (sb.at[1], rb.at[0], (upper, mp)),
            ]
        ):
            out.append(
                pltpu.make_async_remote_copy(
                    src_ref=src, dst_ref=dst, send_sem=xsend.at[base + 2 + i],
                    recv_sem=xrecv.at[base + 2 + i], device_id=to, device_id_type=MESH,
                )
            )
        return out

    def plane_outside(own, rb, members, put):
        used = lax.broadcasted_iota(jnp.int32, (SP, 1), 0) < SLOTS
        received = jnp.concatenate(
            [jnp.where(used, rb[0], 0.0), jnp.where(used, rb[1], 0.0)], axis=0
        )
        if members * FW > received.shape[1]:
            spare = jnp.zeros((2 * SP, FW), F32)
            for m in range(received.shape[1] // FW):
                part = roll(received[:, FW * m : FW * (m + 1)], 7 * m - 25)
                spare = jnp.where((fnode >= 7 * m) & (fnode < 7 * m + 7), part, spare)
            received = jnp.concatenate([received, spare], axis=1)
        got = own + right(hot_recv, received, 3)
        for a in range(2):
            for m in range(members):
                lanes = slice(FW * m, FW * (m + 1))
                lo = got[a * C : (a + 1) * C, lanes]
                hi = got[(2 + a) * C : (3 + a) * C, lanes]
                primal, tangent = swap(lo, hi)
                put(0, m, a, primal)
                put(1, m, a, tangent)

    def layer_outside(blocks, zr, members, put):
        for m in range(members):
            lanes = slice(FW * (m // 2), FW * (m // 2 + 1))
            step = 32 * (L - 1 if m % 2 == 0 else L - 2)
            lo = jnp.where(flayer == 0, roll(zr[0, :, lanes], -step), roll(blocks[2][m][1], 32))
            hi = jnp.where(flayer == L - 1, roll(zr[1, :, lanes], step), roll(blocks[2][m][0], -32))
            primal, tangent = swap(lo, hi)
            put(0, m, 2, primal)
            put(1, m, 2, tangent)

    whole = u[...].reshape(10 * C, VW)
    for a in range(3):
        faces = left(whole, pick_ref[a], 3).reshape(2, 5, C, FW)
        for m in range(5):
            uf[0, m, a] = faces[0, m] + fpad if m % 4 == 0 else faces[0, m]
            uf[1, m, a] = faces[1, m]
    blocks1, table1, sent1, zcopies1 = exchange(
        lambda pt, m, a: uf[pt, m, a], 5, sb1, rb1, zs1, zr1, 0
    )
    pcopies1 = finish_send(sent1, sb1, rb1, 0)
    pl.semaphore_wait(barrier, everyone - 1)
    for copy in pcopies1 + zcopies1:
        copy.start()
    for a in range(3):
        wide = jnp.zeros((C, VW), F32)
        face = jnp.zeros((C, FW), F32)
        for l in range(L):
            value = column(metric_ref[a, l : l + 1, :])
            wide = jnp.where(vl // 128 == l, value, wide)
            face = jnp.where(flayer == l, value, face)
        mv[a] = wide
        mf[a] = face

    for copy in inputs[7:]:
        copy.wait()

    own1 = sum(dot(hot_own, p) for p in table1[::-1])

    @pl.loop(0, C // 8)
    def _(i):
        rows = pl.ds(pl.multiple_of(i * 8, 8), 8)
        primal = [u[0, m, rows, :] for m in range(5)]
        tangent = [u[1, m, rows, :] for m in range(5)]
        fp, ft = jax.jvp(gradient_fields, (primal,), (tangent,))
        for m in range(4):
            w[0, m, rows, :] = fp[m]
            w[1, m, rows, :] = ft[m]

    fields = w[...].reshape(8 * C, VW)
    for a in range(3):
        q[a] = derive(fields, dh_ref[a], dl_ref[a]).reshape(2, 4, C, VW)

    for copy in zcopies1 + pcopies1:
        copy.wait()
    low_wall = jnp.where(source[2] < 0.0, 1.0, 0.0)
    high_wall = jnp.where(source[3] < 0.0, 1.0, 0.0)
    wall = jnp.where(first, low_wall, high_wall) > 0.5

    def put1(pt, m, a, value):
        if a == 1:
            own = uf[pt, m, a]
            value = jnp.where(wall, own if m % 4 == 0 else -own, value)
        of[pt, m, a] = jnp.where(fnode < 25, value, uf[pt, m, a])

    plane_outside(own1, rb1, 5, put1)
    layer_outside(blocks1, zr1, 5, put1)

    for a in range(3):
        @pl.loop(0, C // 8)
        def _(i):
            rows = pl.ds(pl.multiple_of(i * 8, 8), 8)
            primal = ([uf[0, m, a, rows, :] for m in range(5)], [of[0, m, a, rows, :] for m in range(5)])
            tangent = ([uf[1, m, a, rows, :] for m in range(5)], [of[1, m, a, rows, :] for m in range(5)])
            jp, jt = jax.jvp(jump_fields, primal, tangent)
            for m in range(4):
                jf[a, 0, m, rows, :] = (0.5 * LIFT) * sign * jp[m]
                jf[a, 1, m, rows, :] = (0.5 * LIFT) * sign * jt[m]

        q[a] += left(jf[a].reshape(8 * C, FW), lift_ref[a], 2).reshape(2, 4, C, VW)

    @pl.loop(0, C // 8)
    def _(i):
        rows = pl.ds(pl.multiple_of(i * 8, 8), 8)
        scale = [mv[a, rows, :] for a in range(3)]
        states = [[u[pt, m, rows, :] for m in range(5)] for pt in range(2)]
        grads = [
            [[scale[a] * q[a, pt, m, rows, :] for m in range(4)] for a in range(3)]
            for pt in range(2)
        ]
        vp, vt = jax.jvp(viscous_all, (states[0], grads[0]), (states[1], grads[1]))
        for a in range(3):
            for m in range(4):
                v[a, 0, m, rows, :] = vp[a][m]
                v[a, 1, m, rows, :] = vt[a][m]

    for a in range(3):
        vf[a] = left(v[a].reshape(8 * C, VW), pick_ref[a], 3).reshape(2, 4, C, FW)
    blocks2, table2, sent2, zcopies2 = exchange(
        lambda pt, m, a: vf[a, pt, m], 4, sb2, rb2, zs2, zr2, 4
    )
    pcopies2 = finish_send(sent2, sb2, rb2, 4)
    for copy in pcopies2 + zcopies2:
        copy.start()

    own2 = sum(dot(hot_own, p) for p in table2[::-1])

    @pl.loop(0, C // 8)
    def _(i):
        rows = pl.ds(pl.multiple_of(i * 8, 8), 8)
        states = [[u[pt, m, rows, :] for m in range(5)] for pt in range(2)]
        for a in range(3):
            scale = mv[a, rows, :]
            fluxes = jax.jvp(lambda x: inviscid(x, a), (states[0],), (states[1],))
            for pt in range(2):
                g[a, pt, 0, rows, :] = scale * fluxes[pt][0]
                for m in range(4):
                    g[a, pt, m + 1, rows, :] = scale * (fluxes[pt][m + 1] - v[a, pt, m, rows, :])

    for a in range(3):
        @pl.loop(0, C // 8)
        def _(i):
            rows = pl.ds(pl.multiple_of(i * 8, 8), 8)
            primal = ([uf[0, m, a, rows, :] for m in range(5)], [of[0, m, a, rows, :] for m in range(5)])
            tangent = ([uf[1, m, a, rows, :] for m in range(5)], [of[1, m, a, rows, :] for m in range(5)])
            sp, stt = jax.jvp(
                lambda inner, outer: surface(inner, outer, sign, a), primal, tangent
            )
            for m in range(5):
                s[a, 0, m, rows, :] = sp[m]
                s[a, 1, m, rows, :] = stt[m]

    total = None
    for a in range(3):
        part = derive(g[a].reshape(10 * C, VW), dh_ref[a], dl_ref[a])
        total = part if total is None else total + part
    r[...] = total.reshape(2, 5, C, VW)

    for copy in zcopies2 + pcopies2:
        copy.wait()

    def put2(pt, m, a, value):
        if a == 1:
            value = jnp.where(wall, vf[a, pt, m], value)
        ov[a, pt, m] = value

    plane_outside(own2, rb2, 4, put2)
    layer_outside(blocks2, zr2, 4, put2)
    lifted = None
    for a in range(3):
        for pt in range(2):
            s[a, pt, 0] = mf[a] * s[a, pt, 0]
            for m in range(4):
                jump = ov[a, pt, m] - vf[a, pt, m]
                s[a, pt, m + 1] = mf[a] * (s[a, pt, m + 1] - (0.5 * LIFT) * sign * jump)
        part = left(s[a].reshape(10 * C, FW), lift_ref[a], 2)
        lifted = part if lifted is None else lifted + part
    r[...] += lifted.reshape(2, 5, C, VW)

    def whole_sum(parts):
        acc = parts[0]
        for part in parts[1:]:
            acc = acc + part
        return jnp.sum(jnp.sum(acc, axis=0, keepdims=True), axis=1, keepdims=True)

    def ratio(top, bottom):
        return jnp.where(bottom > 0.0, top / jnp.where(bottom > 0.0, bottom, 1.0), 0.0)

    pd = whole_sum([r[1, m] * u[1, m] for m in range(5)])
    dd = whole_sum([u[1, m] * u[1, m] for m in range(5)])
    rs = whole_sum([r[0, m] * r[0, m] for m in range(5)])
    mine = ratio(pd, dd)
    rests = [r[1, m] - mine * u[1, m] for m in range(5)]
    rr = whole_sum([x * x for x in rests])
    rd = whole_sum([x * u[1, m] for m, x in enumerate(rests)])
    lane = lax.broadcasted_iota(jnp.int32, (1, 128), 1)
    row = jnp.zeros((1, 128), F32)
    for i, value in enumerate((pd, dd, rs, rr, rd)):
        row = jnp.where(lane == i, value, row)
    st[...] = row
    copies = [
        pltpu.make_async_remote_copy(
            src_ref=st, dst_ref=sta.at[k], send_sem=asend.at[k], recv_sem=arecv.at[k],
            device_id=peer(k), device_id_type=MESH,
        )
        for k in range(1, everyone)
    ]
    for copy in copies:
        copy.start()
    sta[0] = st[...]
    for l in range(L):
        for m in range(5):
            res_ref[:, l, 125 * m : 125 * (m + 1)] = r[0, m, :, 128 * l : 128 * l + 125]
    for copy in copies:
        copy.wait()
    table = sta[...].reshape(everyone, 128)
    pd, dd, rs, rr, rd = [
        jnp.sum(jnp.where(lane == i, table, 0.0), axis=1, keepdims=True) for i in range(5)
    ]
    coefficient = jnp.sum(pd, axis=0, keepdims=True) * (1.0 / total_count)
    shift = ratio(pd, dd) - coefficient
    rr = jnp.sum(rr + 2.0 * shift * rd + shift * shift * dd, axis=0, keepdims=True)
    rs = jnp.sum(rs, axis=0, keepdims=True)
    beta = jnp.sqrt(rr * (1.0 / total_count))
    norm = jnp.sqrt(rs * (1.0 / total_count))
    kry_ref[...] = jnp.where(lane == 0, coefficient, jnp.where(lane == 1, beta, norm))
    c, inv = coefficient, 1.0 / beta
    for m in range(5):
        value = (r[1, m] - c * u[1, m]) * inv
        for l in range(L):
            basis_ref[:, l, 125 * m : 125 * (m + 1)] = value[:, 128 * l : 128 * l + 125]


def local(ns, np_, state, direction, metric, face_source, send_rows):
    C, L, width = state.shape
    slots = send_rows.shape[2]
    SP = -(-slots // 8) * 8
    VW, FW = 128 * L, 64 * L
    own = 4 * C
    keys = np.full((1, own + 2 * SP), -7, np.int32)
    side, rest = np.divmod(np.arange(own), 2 * C)
    keys[0, :own] = 4 * (rest % C) + 2 * (rest // C) + side
    keys[0, own : own + slots] = own + np.arange(slots)
    keys[0, own + SP : own + SP + slots] = own + slots + np.arange(slots)
    high, low, pick, lift = operators(L)
    operands = (
        state, direction, jnp.transpose(metric, (2, 1, 0)), face_source.T, send_rows,
        *[jnp.asarray(x) for x in (keys, high, low, pick, lift)],
    )
    vmem = lambda *shape: pltpu.VMEM(shape, F32)
    dma = lambda n: pltpu.SemaphoreType.DMA((n,))
    spec = pl.BlockSpec(memory_space=pltpu.VMEM)
    residual, basis, krylov = pl.pallas_call(
        functools.partial(kernel, ns, np_, float(state.size * ns * np_)),
        out_shape=(
            jax.ShapeDtypeStruct(state.shape, F32),
            jax.ShapeDtypeStruct(state.shape, F32),
            jax.ShapeDtypeStruct((1, 128), F32),
        ),
        in_specs=[pl.BlockSpec(memory_space=pltpu.HBM)] * 10,
        out_specs=(spec,) * 3,
        scratch_shapes=[
            vmem(2, 5, C, VW), vmem(2, 5, 3, C, FW), vmem(2, 5, 3, C, FW),
            vmem(2, 4, C, VW), vmem(3, 2, 4, C, FW), vmem(3, 2, 4, C, VW),
            vmem(3, 2, 4, C, VW), vmem(3, 2, 4, C, FW), vmem(3, 2, 4, C, FW),
            vmem(3, 2, 5, C, VW), vmem(3, 2, 5, C, FW), vmem(2, 5, C, VW),
            vmem(3, C, VW), vmem(3, C, FW),
            vmem(2, SP, 4 * FW), vmem(2, SP, 4 * FW), vmem(2, C, 3 * FW), vmem(2, C, 3 * FW),
            vmem(2, SP, 4 * FW), vmem(2, SP, 4 * FW), vmem(2, C, 2 * FW), vmem(2, C, 2 * FW),
            vmem(1, 128), vmem(ns * np_, 1, 128),
            *[pltpu.VMEM(x.shape, x.dtype) for x in operands],
            dma(8), dma(8), dma(ns * np_), dma(ns * np_), dma(10),
        ],
        compiler_params=pltpu.CompilerParams(
            collective_id=0, has_side_effects=True, vmem_limit_bytes=40 * 1024 * 1024
        ),
        name="navier",
    )(*operands)
    return residual, basis, krylov[0, :3]


def solution(mesh):
    return jax.shard_map(
        functools.partial(local, mesh.shape["stream"], mesh.shape["span"]),
        mesh=mesh,
        in_specs=(
            P("stream", "span", None),
            P("stream", "span", None),
            P("stream", "span", None),
            P("stream", None),
            P("stream", None, None),
        ),
        out_specs=(P("stream", "span", None), P("stream", "span", None), P()),
        check_vma=False,
    )
```

```python
import functools
import math

import jax
import jax.numpy as jnp
import numpy as np
from jax import lax
from jax.experimental import pallas as pl
from jax.experimental.pallas import tpu as pltpu
from jax.sharding import PartitionSpec as P

GAMMA = 1.4
VISC = 0.01
COND = VISC * GAMMA / ((GAMMA - 1.0) * 0.72)
LIFT = 10.0
MESH = pl.DeviceIdType.MESH
F32, BF16 = jnp.float32, jnp.bfloat16


def diff_table():
    spread = math.sqrt(3.0 / 7.0)
    points = np.array([-1.0, -spread, 0.0, spread, 1.0])
    weights = np.array(
        [np.prod([points[i] - points[j] for j in range(5) if j != i]) for i in range(5)]
    )
    matrix = np.zeros((5, 5))
    for i in range(5):
        for j in range(5):
            if i != j:
                matrix[i, j] = weights[i] / (weights[j] * (points[i] - points[j]))
        matrix[i, i] = np.sum([1.0 / (points[i] - points[j]) for j in range(5) if j != i])
    return matrix


def operators(layers):
    table = diff_table()
    eye = np.eye(5)
    kron = [
        np.einsum("ai,bj,ck->ijkabc", *[table if m == a else eye for m in range(3)]).reshape(125, 125)
        for a in range(3)
    ]
    node = np.arange(125).reshape(5, 5, 5)
    vw, fw, half = 128 * layers, 64 * layers, 32 * layers
    deriv = np.zeros((3, vw, vw), np.float32)
    pick = np.zeros((3, vw, fw), np.float32)
    for a in range(3):
        for l in range(layers):
            b = 128 * l
            deriv[a, b : b + 125, b : b + 125] = kron[a]
            for side in range(2):
                face = np.take(node, 4 * side, axis=a).reshape(-1)
                for m, at in enumerate(face):
                    pick[a, b + at, side * half + 32 * l + m] = 1.0
    high = deriv.astype(jnp.bfloat16)
    low = (deriv - high.astype(np.float32)).astype(jnp.bfloat16)
    lift = np.swapaxes(pick, 1, 2)
    return high, low, pick.astype(jnp.bfloat16), lift.astype(jnp.bfloat16)


def pieces(x, n):
    out = []
    for i in range(n):
        p = x.astype(BF16)
        out.append(p)
        if i + 1 < n:
            x = x - p.astype(F32)
    return out


def dot(a, b):
    return jnp.dot(a, b, preferred_element_type=F32)


def left(x, w, n):
    return sum(dot(p, w) for p in pieces(x, n)[::-1])


def right(w, x, n):
    return sum(dot(w, p) for p in pieces(x, n)[::-1])


def derive(x, high, low):
    a, b = pieces(x, 2)
    return dot(a, low) + dot(b, high) + dot(a, high)


def fields_of(u):
    inv = 1.0 / u[0]
    vel = [u[1] * inv, u[2] * inv, u[3] * inv]
    kinetic = 0.5 * (u[1] * vel[0] + u[2] * vel[1] + u[3] * vel[2])
    pressure = (GAMMA - 1.0) * (u[4] - kinetic)
    return vel, pressure, pressure * inv


def inviscid(u, a):
    vel, pressure, _ = fields_of(u)
    out = [u[1 + a]]
    for m in range(3):
        term = u[1 + m] * vel[a]
        out.append(term + pressure if m == a else term)
    out.append((u[4] + pressure) * vel[a])
    return out


def viscous(vel, q, a, divergence):
    stress = []
    for m in range(3):
        term = q[a][m] + q[m][a]
        if m == a:
            term = term - 2.0 / 3.0 * divergence
        stress.append(VISC * term)
    energy = stress[0] * vel[0] + stress[1] * vel[1] + stress[2] * vel[2] + COND * q[a][3]
    return stress + [energy]


def viscous_all(u, q):
    inv = 1.0 / u[0]
    vel = [u[1] * inv, u[2] * inv, u[3] * inv]
    divergence = q[0][0] + q[1][1] + q[2][2]
    return [viscous(vel, q, a, divergence) for a in range(3)]


def gradient_fields(u):
    vel, _, temper = fields_of(u)
    return vel + [temper]


def jump_fields(inner, outer):
    return [o - i for o, i in zip(gradient_fields(outer), gradient_fields(inner))]


def surface(inner, outer, sign, a):
    vi, pi, ti = fields_of(inner)
    vo, po, to = fields_of(outer)
    square = sum(v * v for v in vi) + GAMMA * ti + sum(v * v for v in vo) + GAMMA * to
    speed = jnp.sqrt(0.5 * square)
    fi, fo = inviscid(inner, a), inviscid(outer, a)
    return [
        (0.5 * LIFT) * (sign * (fo[m] - fi[m]) - speed * (outer[m] - inner[m])) for m in range(5)
    ]


def kernel(
    ns, np_, total_count,
    x_hbm, d_hbm, metric_hbm, fs_hbm, sr_hbm, key_hbm, dh_hbm, dl_hbm, pick_hbm, lift_hbm,
    res_ref, basis_ref, kry_ref,
    u, uf, of, w, jf, q, v, vf, ov, g, s, r, mv, mf,
    sb1, rb1, zs1, zr1, sb2, rb2, zs2, zr2, st, sta,
    x_ref, d_ref, metric_ref, fs_ref, sr_ref, keyrow_ref, dh_ref, dl_ref, pick_ref, lift_ref,
    xsend, xrecv, asend, arecv, loads,
):
    C, L = x_ref.shape[0], x_ref.shape[1]
    VW, FW, half = 128 * L, 64 * L, 32 * L
    SLOTS = sr_ref.shape[2]
    SP = sb1.shape[1]
    OWN = 4 * C
    ms, mp = lax.axis_index("stream"), lax.axis_index("span")
    lower, upper = lax.rem(ms + ns - 1, ns), lax.rem(ms + 1, ns)
    below, above = lax.rem(mp + np_ - 1, np_), lax.rem(mp + 1, np_)

    inputs = [
        pltpu.make_async_copy(src, dst, loads.at[i])
        for i, (src, dst) in enumerate(
            [
                (x_hbm, x_ref), (d_hbm, d_ref), (pick_hbm, pick_ref), (key_hbm, keyrow_ref),
                (fs_hbm, fs_ref), (sr_hbm, sr_ref), (metric_hbm, metric_ref),
                (dh_hbm, dh_ref), (dl_hbm, dl_ref), (lift_hbm, lift_ref),
            ]
        )
    ]
    for copy in inputs:
        copy.start()

    def peer(k):
        a, b = divmod(k, np_)
        return lax.rem(ms + a, ns), lax.rem(mp + b, np_)

    everyone = ns * np_
    barrier = pltpu.get_barrier_semaphore()
    for k in range(1, everyone):
        pl.semaphore_signal(barrier, inc=1, device_id=peer(k), device_id_type=MESH)

    fl = lax.broadcasted_iota(jnp.int32, (1, FW), 1)
    vl = lax.broadcasted_iota(jnp.int32, (1, VW), 1)
    first = fl < half
    sign = jnp.where(first, -1.0, 1.0)
    flayer = lax.rem(fl, half) // 32
    fnode = lax.rem(fl, 32)
    fpad = jnp.where(fnode >= 25, 1.0, 0.0)

    def roll(x, shift):
        shift = shift % FW
        return pltpu.roll(x, shift, 1) if shift else x

    di = lax.broadcasted_iota(jnp.int32, (C, C), 0)
    dj = lax.broadcasted_iota(jnp.int32, (C, C), 1)

    def column(row):
        return jnp.sum(jnp.where(di == dj, row, 0.0), axis=1, keepdims=True)

    for copy in inputs[:2]:
        copy.wait()

    for pt, ref in enumerate((x_ref, d_ref)):
        for l in range(L):
            for m in range(5):
                pad = 1.0 if pt == 0 and m % 4 == 0 else 0.0
                u[pt, m, :, 128 * l + 120 : 128 * (l + 1)] = jnp.full((C, 8), pad, F32)
                u[pt, m, :, 128 * l : 128 * l + 125] = ref[:, l, 125 * m : 125 * (m + 1)]
    for copy in inputs[2:7]:
        copy.wait()
    keyrow = keyrow_ref[...].astype(F32)
    source = [column(fs_ref[f : f + 1, :].astype(F32)) for f in range(4)]
    onehot = jnp.concatenate(
        [
            jnp.where(source[2 * a + side] == keyrow, 1.0, 0.0)
            for side in range(2)
            for a in range(2)
        ],
        axis=0,
    ).astype(BF16)
    hot_own, hot_recv = onehot[:, :OWN], onehot[:, OWN : OWN + 2 * SP]
    ri = lax.broadcasted_iota(jnp.int32, (SP, SLOTS), 0)
    li = lax.broadcasted_iota(jnp.int32, (SP, SLOTS), 1)
    send_hot = []
    for side in range(2):
        row = sr_ref[0, side : side + 1, :].astype(F32)
        wanted = jnp.sum(jnp.where(ri == li, row, 0.0), axis=1, keepdims=True)
        send_hot.append(jnp.where(wanted == keyrow[:, :OWN], 1.0, 0.0))
    send_hot = jnp.concatenate(send_hot, axis=0).astype(BF16)

    def swap(a, b):
        return (
            jnp.where(first, a, pltpu.roll(b, half, 1)),
            jnp.where(first, pltpu.roll(a, half, 1), b),
        )

    def exchange(faces, members, sb, rb, zs, zr, base):
        blocks = [[swap(faces(0, m, a), faces(1, m, a)) for m in range(members)] for a in range(3)]
        table = jnp.concatenate(
            [
                jnp.concatenate([blocks[a][m][side] for m in range(members)], axis=1)
                for side in range(2)
                for a in range(2)
            ],
            axis=0,
        )
        for m in range(0, members, 2):
            for side in range(2):
                value = blocks[2][m][side]
                if m + 1 < members:
                    other = roll(blocks[2][m + 1][side], 32 if side == 0 else -32)
                    value = jnp.where(flayer == (0 if side == 0 else L - 1), value, other)
                zs[side, :, FW * (m // 2) : FW * (m // 2 + 1)] = value
        zs_copies = [
            (zs.at[0], zr.at[1], (ms, below)),
            (zs.at[1], zr.at[0], (ms, above)),
        ]
        copies = []
        for i, (src, dst, to) in enumerate(zs_copies):
            copies.append(
                pltpu.make_async_remote_copy(
                    src_ref=src, dst_ref=dst, send_sem=xsend.at[base + i],
                    recv_sem=xrecv.at[base + i], device_id=to, device_id_type=MESH,
                )
            )
        table_pieces = pieces(table, 3)
        sent = sum(dot(send_hot, p) for p in table_pieces[::-1])
        return blocks, table_pieces, sent, copies

    def finish_send(sent, sb, rb, base):
        width = sb.shape[2]
        for m in range(width // FW):
            value = sent[:, FW * m : FW * (m + 1)]
            if sent.shape[1] > width:
                spare = roll(sent[:, width:], 25 - 7 * m)
                value = jnp.where(fnode < 25, value, spare)
            sb[0, :, FW * m : FW * (m + 1)] = value[:SP]
            sb[1, :, FW * m : FW * (m + 1)] = value[SP:]
        out = []
        for i, (src, dst, to) in enumerate(
            [
                (sb.at[0], rb.at[1], (lower, mp)),
                (sb.at[1], rb.at[0], (upper, mp)),
            ]
        ):
            out.append(
                pltpu.make_async_remote_copy(
                    src_ref=src, dst_ref=dst, send_sem=xsend.at[base + 2 + i],
                    recv_sem=xrecv.at[base + 2 + i], device_id=to, device_id_type=MESH,
                )
            )
        return out

    def plane_outside(own, rb, members, put):
        used = lax.broadcasted_iota(jnp.int32, (SP, 1), 0) < SLOTS
        received = jnp.concatenate(
            [jnp.where(used, rb[0], 0.0), jnp.where(used, rb[1], 0.0)], axis=0
        )
        if members * FW > received.shape[1]:
            spare = jnp.zeros((2 * SP, FW), F32)
            for m in range(received.shape[1] // FW):
                part = roll(received[:, FW * m : FW * (m + 1)], 7 * m - 25)
                spare = jnp.where((fnode >= 7 * m) & (fnode < 7 * m + 7), part, spare)
            received = jnp.concatenate([received, spare], axis=1)
        got = own + right(hot_recv, received, 3)
        for a in range(2):
            for m in range(members):
                lanes = slice(FW * m, FW * (m + 1))
                lo = got[a * C : (a + 1) * C, lanes]
                hi = got[(2 + a) * C : (3 + a) * C, lanes]
                primal, tangent = swap(lo, hi)
                put(0, m, a, primal)
                put(1, m, a, tangent)

    def layer_outside(blocks, zr, members, put):
        for m in range(members):
            lanes = slice(FW * (m // 2), FW * (m // 2 + 1))
            step = 32 * (L - 1 if m % 2 == 0 else L - 2)
            lo = jnp.where(flayer == 0, roll(zr[0, :, lanes], -step), roll(blocks[2][m][1], 32))
            hi = jnp.where(flayer == L - 1, roll(zr[1, :, lanes], step), roll(blocks[2][m][0], -32))
            primal, tangent = swap(lo, hi)
            put(0, m, 2, primal)
            put(1, m, 2, tangent)

    whole = u[...].reshape(10 * C, VW)
    for a in range(3):
        faces = left(whole, pick_ref[a], 3).reshape(2, 5, C, FW)
        for m in range(5):
            uf[0, m, a] = faces[0, m] + fpad if m % 4 == 0 else faces[0, m]
            uf[1, m, a] = faces[1, m]
    blocks1, table1, sent1, zcopies1 = exchange(
        lambda pt, m, a: uf[pt, m, a], 5, sb1, rb1, zs1, zr1, 0
    )
    pcopies1 = finish_send(sent1, sb1, rb1, 0)
    pl.semaphore_wait(barrier, everyone - 1)
    for copy in pcopies1 + zcopies1:
        copy.start()
    for a in range(3):
        wide = jnp.zeros((C, VW), F32)
        face = jnp.zeros((C, FW), F32)
        for l in range(L):
            value = column(metric_ref[a, l : l + 1, :])
            wide = jnp.where(vl // 128 == l, value, wide)
            face = jnp.where(flayer == l, value, face)
        mv[a] = wide
        mf[a] = face

    for copy in inputs[7:]:
        copy.wait()

    own1 = sum(dot(hot_own, p) for p in table1[::-1])

    @pl.loop(0, C // 8)
    def _(i):
        rows = pl.ds(pl.multiple_of(i * 8, 8), 8)
        primal = [u[0, m, rows, :] for m in range(5)]
        tangent = [u[1, m, rows, :] for m in range(5)]
        fp, ft = jax.jvp(gradient_fields, (primal,), (tangent,))
        for m in range(4):
            w[0, m, rows, :] = fp[m]
            w[1, m, rows, :] = ft[m]

    fields = w[...].reshape(8 * C, VW)
    for a in range(3):
        q[a] = derive(fields, dh_ref[a], dl_ref[a]).reshape(2, 4, C, VW)

    for copy in zcopies1 + pcopies1:
        copy.wait()
    low_wall = jnp.where(source[2] < 0.0, 1.0, 0.0)
    high_wall = jnp.where(source[3] < 0.0, 1.0, 0.0)
    wall = jnp.where(first, low_wall, high_wall) > 0.5

    def put1(pt, m, a, value):
        if a == 1:
            own = uf[pt, m, a]
            value = jnp.where(wall, own if m % 4 == 0 else -own, value)
        of[pt, m, a] = jnp.where(fnode < 25, value, uf[pt, m, a])

    plane_outside(own1, rb1, 5, put1)
    layer_outside(blocks1, zr1, 5, put1)

    for a in range(3):
        @pl.loop(0, C // 8)
        def _(i):
            rows = pl.ds(pl.multiple_of(i * 8, 8), 8)
            primal = ([uf[0, m, a, rows, :] for m in range(5)], [of[0, m, a, rows, :] for m in range(5)])
            tangent = ([uf[1, m, a, rows, :] for m in range(5)], [of[1, m, a, rows, :] for m in range(5)])
            jp, jt = jax.jvp(jump_fields, primal, tangent)
            for m in range(4):
                jf[a, 0, m, rows, :] = (0.5 * LIFT) * sign * jp[m]
                jf[a, 1, m, rows, :] = (0.5 * LIFT) * sign * jt[m]

        q[a] += left(jf[a].reshape(8 * C, FW), lift_ref[a], 2).reshape(2, 4, C, VW)

    @pl.loop(0, C // 8)
    def _(i):
        rows = pl.ds(pl.multiple_of(i * 8, 8), 8)
        scale = [mv[a, rows, :] for a in range(3)]
        states = [[u[pt, m, rows, :] for m in range(5)] for pt in range(2)]
        grads = [
            [[scale[a] * q[a, pt, m, rows, :] for m in range(4)] for a in range(3)]
            for pt in range(2)
        ]
        vp, vt = jax.jvp(viscous_all, (states[0], grads[0]), (states[1], grads[1]))
        for a in range(3):
            for m in range(4):
                v[a, 0, m, rows, :] = vp[a][m]
                v[a, 1, m, rows, :] = vt[a][m]

    for a in range(3):
        vf[a] = left(v[a].reshape(8 * C, VW), pick_ref[a], 3).reshape(2, 4, C, FW)
    blocks2, table2, sent2, zcopies2 = exchange(
        lambda pt, m, a: vf[a, pt, m], 4, sb2, rb2, zs2, zr2, 4
    )
    pcopies2 = finish_send(sent2, sb2, rb2, 4)
    for copy in pcopies2 + zcopies2:
        copy.start()

    own2 = sum(dot(hot_own, p) for p in table2[::-1])

    @pl.loop(0, C // 8)
    def _(i):
        rows = pl.ds(pl.multiple_of(i * 8, 8), 8)
        states = [[u[pt, m, rows, :] for m in range(5)] for pt in range(2)]
        for a in range(3):
            scale = mv[a, rows, :]
            fluxes = jax.jvp(lambda x: inviscid(x, a), (states[0],), (states[1],))
            for pt in range(2):
                g[a, pt, 0, rows, :] = scale * fluxes[pt][0]
                for m in range(4):
                    g[a, pt, m + 1, rows, :] = scale * (fluxes[pt][m + 1] - v[a, pt, m, rows, :])

    for a in range(3):
        @pl.loop(0, C // 8)
        def _(i):
            rows = pl.ds(pl.multiple_of(i * 8, 8), 8)
            primal = ([uf[0, m, a, rows, :] for m in range(5)], [of[0, m, a, rows, :] for m in range(5)])
            tangent = ([uf[1, m, a, rows, :] for m in range(5)], [of[1, m, a, rows, :] for m in range(5)])
            sp, stt = jax.jvp(
                lambda inner, outer: surface(inner, outer, sign, a), primal, tangent
            )
            for m in range(5):
                s[a, 0, m, rows, :] = sp[m]
                s[a, 1, m, rows, :] = stt[m]

    total = None
    for a in range(3):
        part = derive(g[a].reshape(10 * C, VW), dh_ref[a], dl_ref[a])
        total = part if total is None else total + part
    r[...] = total.reshape(2, 5, C, VW)

    for copy in zcopies2 + pcopies2:
        copy.wait()

    def put2(pt, m, a, value):
        if a == 1:
            value = jnp.where(wall, vf[a, pt, m], value)
        ov[a, pt, m] = value

    plane_outside(own2, rb2, 4, put2)
    layer_outside(blocks2, zr2, 4, put2)
    lifted = None
    for a in range(3):
        for pt in range(2):
            s[a, pt, 0] = mf[a] * s[a, pt, 0]
            for m in range(4):
                jump = ov[a, pt, m] - vf[a, pt, m]
                s[a, pt, m + 1] = mf[a] * (s[a, pt, m + 1] - (0.5 * LIFT) * sign * jump)
        part = left(s[a].reshape(10 * C, FW), lift_ref[a], 2)
        lifted = part if lifted is None else lifted + part
    r[...] += lifted.reshape(2, 5, C, VW)

    def whole_sum(parts):
        acc = parts[0]
        for part in parts[1:]:
            acc = acc + part
        return jnp.sum(jnp.sum(acc, axis=0, keepdims=True), axis=1, keepdims=True)

    def ratio(top, bottom):
        return jnp.where(bottom > 0.0, top / jnp.where(bottom > 0.0, bottom, 1.0), 0.0)

    pd = whole_sum([r[1, m] * u[1, m] for m in range(5)])
    dd = whole_sum([u[1, m] * u[1, m] for m in range(5)])
    rs = whole_sum([r[0, m] * r[0, m] for m in range(5)])
    mine = ratio(pd, dd)
    rests = [r[1, m] - mine * u[1, m] for m in range(5)]
    rr = whole_sum([x * x for x in rests])
    rd = whole_sum([x * u[1, m] for m, x in enumerate(rests)])
    lane = lax.broadcasted_iota(jnp.int32, (1, 128), 1)
    row = jnp.zeros((1, 128), F32)
    for i, value in enumerate((pd, dd, rs, rr, rd)):
        row = jnp.where(lane == i, value, row)
    st[...] = row
    copies = [
        pltpu.make_async_remote_copy(
            src_ref=st, dst_ref=sta.at[k], send_sem=asend.at[k], recv_sem=arecv.at[k],
            device_id=peer(k), device_id_type=MESH,
        )
        for k in range(1, everyone)
    ]
    for copy in copies:
        copy.start()
    sta[0] = st[...]
    for l in range(L):
        for m in range(5):
            res_ref[:, l, 125 * m : 125 * (m + 1)] = r[0, m, :, 128 * l : 128 * l + 125]
    for copy in copies:
        copy.wait()
    table = sta[...].reshape(everyone, 128)
    pd, dd, rs, rr, rd = [
        jnp.sum(jnp.where(lane == i, table, 0.0), axis=1, keepdims=True) for i in range(5)
    ]
    coefficient = jnp.sum(pd, axis=0, keepdims=True) * (1.0 / total_count)
    shift = ratio(pd, dd) - coefficient
    rr = jnp.sum(rr + 2.0 * shift * rd + shift * shift * dd, axis=0, keepdims=True)
    rs = jnp.sum(rs, axis=0, keepdims=True)
    beta = jnp.sqrt(rr * (1.0 / total_count))
    norm = jnp.sqrt(rs * (1.0 / total_count))
    kry_ref[...] = jnp.where(lane == 0, coefficient, jnp.where(lane == 1, beta, norm))
    c, inv = coefficient, 1.0 / beta
    for m in range(5):
        value = (r[1, m] - c * u[1, m]) * inv
        for l in range(L):
            basis_ref[:, l, 125 * m : 125 * (m + 1)] = value[:, 128 * l : 128 * l + 125]


def local(ns, np_, state, direction, metric, face_source, send_rows):
    C, L, width = state.shape
    slots = send_rows.shape[2]
    SP = -(-slots // 8) * 8
    VW, FW = 128 * L, 64 * L
    own = 4 * C
    keys = np.full((1, own + 2 * SP), -7, np.int32)
    side, rest = np.divmod(np.arange(own), 2 * C)
    keys[0, :own] = 4 * (rest % C) + 2 * (rest // C) + side
    keys[0, own : own + slots] = own + np.arange(slots)
    keys[0, own + SP : own + SP + slots] = own + slots + np.arange(slots)
    high, low, pick, lift = operators(L)
    operands = (
        state, direction, jnp.transpose(metric, (2, 1, 0)), face_source.T, send_rows,
        *[jnp.asarray(x) for x in (keys, high, low, pick, lift)],
    )
    vmem = lambda *shape: pltpu.VMEM(shape, F32)
    dma = lambda n: pltpu.SemaphoreType.DMA((n,))
    spec = pl.BlockSpec(memory_space=pltpu.VMEM)
    residual, basis, krylov = pl.pallas_call(
        functools.partial(kernel, ns, np_, float(state.size * ns * np_)),
        out_shape=(
            jax.ShapeDtypeStruct(state.shape, F32),
            jax.ShapeDtypeStruct(state.shape, F32),
            jax.ShapeDtypeStruct((1, 128), F32),
        ),
        in_specs=[pl.BlockSpec(memory_space=pltpu.HBM)] * 10,
        out_specs=(spec,) * 3,
        scratch_shapes=[
            vmem(2, 5, C, VW), vmem(2, 5, 3, C, FW), vmem(2, 5, 3, C, FW),
            vmem(2, 4, C, VW), vmem(3, 2, 4, C, FW), vmem(3, 2, 4, C, VW),
            vmem(3, 2, 4, C, VW), vmem(3, 2, 4, C, FW), vmem(3, 2, 4, C, FW),
            vmem(3, 2, 5, C, VW), vmem(3, 2, 5, C, FW), vmem(2, 5, C, VW),
            vmem(3, C, VW), vmem(3, C, FW),
            vmem(2, SP, 4 * FW), vmem(2, SP, 4 * FW), vmem(2, C, 3 * FW), vmem(2, C, 3 * FW),
            vmem(2, SP, 4 * FW), vmem(2, SP, 4 * FW), vmem(2, C, 2 * FW), vmem(2, C, 2 * FW),
            vmem(1, 128), vmem(ns * np_, 1, 128),
            *[pltpu.VMEM(x.shape, x.dtype) for x in operands],
            dma(8), dma(8), dma(ns * np_), dma(ns * np_), dma(10),
        ],
        compiler_params=pltpu.CompilerParams(
            collective_id=0, has_side_effects=True, vmem_limit_bytes=63 * 1024 * 1024
        ),
        name="navier",
    )(*operands)
    return residual, basis, krylov[0, :3]


def solution(mesh):
    return jax.shard_map(
        functools.partial(local, mesh.shape["stream"], mesh.shape["span"]),
        mesh=mesh,
        in_specs=(
            P("stream", "span", None),
            P("stream", "span", None),
            P("stream", "span", None),
            P("stream", None),
            P("stream", None, None),
        ),
        out_specs=(P("stream", "span", None), P("stream", "span", None), P()),
        check_vma=False,
    )
```

```python
import functools
import math

import jax
import jax.numpy as jnp
import numpy as np
from jax import lax
from jax.experimental import pallas as pl
from jax.experimental.pallas import tpu as pltpu
from jax.sharding import PartitionSpec as P

GAMMA = 1.4
VISC = 0.01
COND = VISC * GAMMA / ((GAMMA - 1.0) * 0.72)
LIFT = 10.0
MESH = pl.DeviceIdType.MESH
F32, BF16 = jnp.float32, jnp.bfloat16


def diff_table():
    spread = math.sqrt(3.0 / 7.0)
    points = np.array([-1.0, -spread, 0.0, spread, 1.0])
    weights = np.array(
        [np.prod([points[i] - points[j] for j in range(5) if j != i]) for i in range(5)]
    )
    matrix = np.zeros((5, 5))
    for i in range(5):
        for j in range(5):
            if i != j:
                matrix[i, j] = weights[i] / (weights[j] * (points[i] - points[j]))
        matrix[i, i] = np.sum([1.0 / (points[i] - points[j]) for j in range(5) if j != i])
    return matrix


def operators(layers):
    table = diff_table()
    eye = np.eye(5)
    kron = [
        np.einsum("ai,bj,ck->ijkabc", *[table if m == a else eye for m in range(3)]).reshape(125, 125)
        for a in range(3)
    ]
    node = np.arange(125).reshape(5, 5, 5)
    vw, fw, half = 128 * layers, 64 * layers, 32 * layers
    deriv = np.zeros((3, vw, vw), np.float32)
    pick = np.zeros((3, vw, fw), np.float32)
    for a in range(3):
        for l in range(layers):
            b = 128 * l
            deriv[a, b : b + 125, b : b + 125] = kron[a]
            for side in range(2):
                face = np.take(node, 4 * side, axis=a).reshape(-1)
                for m, at in enumerate(face):
                    pick[a, b + at, side * half + 32 * l + m] = 1.0
    high = deriv.astype(jnp.bfloat16)
    low = (deriv - high.astype(np.float32)).astype(jnp.bfloat16)
    lift = np.swapaxes(pick, 1, 2)
    return high, low, pick.astype(jnp.bfloat16), lift.astype(jnp.bfloat16)


def pieces(x, n):
    out = []
    for i in range(n):
        p = x.astype(BF16)
        out.append(p)
        if i + 1 < n:
            x = x - p.astype(F32)
    return out


def dot(a, b):
    return jnp.dot(a, b, preferred_element_type=F32)


def left(x, w, n):
    return sum(dot(p, w) for p in pieces(x, n)[::-1])


def right(w, x, n):
    return sum(dot(w, p) for p in pieces(x, n)[::-1])


def derive(x, high, low):
    a, b = pieces(x, 2)
    return dot(a, low) + dot(b, high) + dot(a, high)


def fields_of(u):
    inv = 1.0 / u[0]
    vel = [u[1] * inv, u[2] * inv, u[3] * inv]
    kinetic = 0.5 * (u[1] * vel[0] + u[2] * vel[1] + u[3] * vel[2])
    pressure = (GAMMA - 1.0) * (u[4] - kinetic)
    return vel, pressure, pressure * inv


def inviscid(u, a):
    vel, pressure, _ = fields_of(u)
    out = [u[1 + a]]
    for m in range(3):
        term = u[1 + m] * vel[a]
        out.append(term + pressure if m == a else term)
    out.append((u[4] + pressure) * vel[a])
    return out


def viscous(vel, q, a, divergence):
    stress = []
    for m in range(3):
        term = q[a][m] + q[m][a]
        if m == a:
            term = term - 2.0 / 3.0 * divergence
        stress.append(VISC * term)
    energy = stress[0] * vel[0] + stress[1] * vel[1] + stress[2] * vel[2] + COND * q[a][3]
    return stress + [energy]


def viscous_all(u, q):
    inv = 1.0 / u[0]
    vel = [u[1] * inv, u[2] * inv, u[3] * inv]
    divergence = q[0][0] + q[1][1] + q[2][2]
    return [viscous(vel, q, a, divergence) for a in range(3)]


def gradient_fields(u):
    vel, _, temper = fields_of(u)
    return vel + [temper]


def jump_fields(inner, outer):
    return [o - i for o, i in zip(gradient_fields(outer), gradient_fields(inner))]


def surface(inner, outer, sign, a):
    vi, pi, ti = fields_of(inner)
    vo, po, to = fields_of(outer)
    square = sum(v * v for v in vi) + GAMMA * ti + sum(v * v for v in vo) + GAMMA * to
    speed = jnp.sqrt(0.5 * square)
    fi, fo = inviscid(inner, a), inviscid(outer, a)
    return [
        (0.5 * LIFT) * (sign * (fo[m] - fi[m]) - speed * (outer[m] - inner[m])) for m in range(5)
    ]


def kernel(
    ns, np_, total_count,
    x_hbm, d_hbm, metric_hbm, fs_hbm, sr_hbm, key_hbm, dh_hbm, dl_hbm, pick_hbm, lift_hbm,
    res_ref, basis_ref, kry_ref,
    u, uf, of, w, jf, q, v, vf, ov, g, s, r, mv, mf,
    sb1, rb1, zs1, zr1, sb2, rb2, zs2, zr2, st, sta,
    x_ref, d_ref, metric_ref, fs_ref, sr_ref, keyrow_ref, dh_ref, dl_ref, pick_ref, lift_ref,
    xsend, xrecv, asend, arecv, loads,
):
    C, L = x_ref.shape[0], x_ref.shape[1]
    VW, FW, half = 128 * L, 64 * L, 32 * L
    SLOTS = sr_ref.shape[2]
    SP = -(-SLOTS // 8) * 8
    MAIN, REM = SLOTS // 8, SLOTS % 8
    OWN = 4 * C
    ms, mp = lax.axis_index("stream"), lax.axis_index("span")
    lower, upper = lax.rem(ms + ns - 1, ns), lax.rem(ms + 1, ns)
    below, above = lax.rem(mp + np_ - 1, np_), lax.rem(mp + 1, np_)

    inputs = [
        pltpu.make_async_copy(src, dst, loads.at[i])
        for i, (src, dst) in enumerate(
            [
                (x_hbm, x_ref), (d_hbm, d_ref), (pick_hbm, pick_ref), (key_hbm, keyrow_ref),
                (fs_hbm, fs_ref), (sr_hbm, sr_ref), (metric_hbm, metric_ref),
                (dh_hbm, dh_ref), (dl_hbm, dl_ref), (lift_hbm, lift_ref),
            ]
        )
    ]
    for copy in inputs:
        copy.start()

    def peer(k):
        a, b = divmod(k, np_)
        return lax.rem(ms + a, ns), lax.rem(mp + b, np_)

    everyone = ns * np_
    barrier = pltpu.get_barrier_semaphore()
    for k in range(1, everyone):
        pl.semaphore_signal(barrier, inc=1, device_id=peer(k), device_id_type=MESH)

    fl = lax.broadcasted_iota(jnp.int32, (1, FW), 1)
    vl = lax.broadcasted_iota(jnp.int32, (1, VW), 1)
    first = fl < half
    sign = jnp.where(first, -1.0, 1.0)
    flayer = lax.rem(fl, half) // 32
    fnode = lax.rem(fl, 32)
    fpad = jnp.where(fnode >= 25, 1.0, 0.0)

    def roll(x, shift):
        shift = shift % FW
        return pltpu.roll(x, shift, 1) if shift else x

    di = lax.broadcasted_iota(jnp.int32, (C, C), 0)
    dj = lax.broadcasted_iota(jnp.int32, (C, C), 1)

    def column(row):
        return jnp.sum(jnp.where(di == dj, row, 0.0), axis=1, keepdims=True)

    for copy in inputs[:2]:
        copy.wait()

    for pt, ref in enumerate((x_ref, d_ref)):
        for l in range(L):
            for m in range(5):
                pad = 1.0 if pt == 0 and m % 4 == 0 else 0.0
                u[pt, m, :, 128 * l + 120 : 128 * (l + 1)] = jnp.full((C, 8), pad, F32)
                u[pt, m, :, 128 * l : 128 * l + 125] = ref[:, l, 125 * m : 125 * (m + 1)]
    for copy in inputs[2:7]:
        copy.wait()
    keyrow = keyrow_ref[...].astype(F32)
    source = [column(fs_ref[f : f + 1, :].astype(F32)) for f in range(4)]
    onehot = jnp.concatenate(
        [
            jnp.where(source[2 * a + side] == keyrow, 1.0, 0.0)
            for side in range(2)
            for a in range(2)
        ],
        axis=0,
    ).astype(BF16)
    hot_own, hot_recv = onehot[:, :OWN], onehot[:, OWN : OWN + 2 * SP]
    ri = lax.broadcasted_iota(jnp.int32, (SP, SLOTS), 0)
    li = lax.broadcasted_iota(jnp.int32, (SP, SLOTS), 1)
    send_hot = []
    for side in range(2):
        row = sr_ref[0, side : side + 1, :].astype(F32)
        wanted = jnp.sum(jnp.where(ri == li, row, 0.0), axis=1, keepdims=True)
        send_hot.append(jnp.where(wanted == keyrow[:, :OWN], 1.0, 0.0))
    send_hot = jnp.concatenate(send_hot, axis=0).astype(BF16)

    def swap(a, b):
        return (
            jnp.where(first, a, pltpu.roll(b, half, 1)),
            jnp.where(first, pltpu.roll(a, half, 1), b),
        )

    def exchange(faces, members, sb, rb, zs, zr, base):
        blocks = [[swap(faces(0, m, a), faces(1, m, a)) for m in range(members)] for a in range(3)]
        table = jnp.concatenate(
            [
                jnp.concatenate([blocks[a][m][side] for m in range(members)], axis=1)
                for side in range(2)
                for a in range(2)
            ],
            axis=0,
        )
        for m in range(0, members, 2):
            for side in range(2):
                value = blocks[2][m][side]
                if m + 1 < members:
                    other = roll(blocks[2][m + 1][side], 32 if side == 0 else -32)
                    value = jnp.where(flayer == (0 if side == 0 else L - 1), value, other)
                zs[side, :, FW * (m // 2) : FW * (m // 2 + 1)] = value
        zs_copies = [
            (zs.at[0], zr.at[1], (ms, below)),
            (zs.at[1], zr.at[0], (ms, above)),
        ]
        copies = []
        for i, (src, dst, to) in enumerate(zs_copies):
            copies.append(
                pltpu.make_async_remote_copy(
                    src_ref=src, dst_ref=dst, send_sem=xsend.at[base + i],
                    recv_sem=xrecv.at[base + i], device_id=to, device_id_type=MESH,
                )
            )
        table_pieces = pieces(table, 3)
        sent = sum(dot(send_hot, p) for p in table_pieces[::-1])
        return blocks, table_pieces, sent, copies

    def finish_send(sent, sb, rb, base):
        for m in range(4):
            value = sent[:, FW * m : FW * (m + 1)]
            if sent.shape[1] > 4 * FW:
                spare = roll(sent[:, 4 * FW :], 25 - 7 * m)
                value = jnp.where(fnode < 25, value, spare)
            for side in range(2):
                for b in range(MAIN):
                    at = side * SP + 8 * b
                    sb[side, 4 * b + m] = value[at : at + 8]
                for e in range(REM):
                    at, to = side * SP + 8 * MAIN + e, REM * m + e
                    sb[side, 4 * MAIN + to // 8, to % 8 : to % 8 + 1, :] = value[at : at + 1]
        out = []
        for i, (src, dst, to) in enumerate(
            [
                (sb.at[0], rb.at[1], (lower, mp)),
                (sb.at[1], rb.at[0], (upper, mp)),
            ]
        ):
            out.append(
                pltpu.make_async_remote_copy(
                    src_ref=src, dst_ref=dst, send_sem=xsend.at[base + 2 + i],
                    recv_sem=xrecv.at[base + 2 + i], device_id=to, device_id_type=MESH,
                )
            )
        return out

    def plane_outside(own, rb, members, put):
        row8 = lax.broadcasted_iota(jnp.int32, (8, 1), 0)
        rows = []
        for side in range(2):
            rows += [
                jnp.concatenate([rb[side, 4 * b + m] for m in range(4)], axis=1)
                for b in range(MAIN)
            ]
            if REM:
                parts = []
                for m in range(4):
                    part = jnp.zeros((8, FW), F32)
                    for e in range(REM):
                        to = REM * m + e
                        line = rb[side, 4 * MAIN + to // 8, to % 8 : to % 8 + 1, :]
                        part = jnp.where(row8 == e, line, part)
                    parts.append(part)
                rows.append(jnp.concatenate(parts, axis=1))
        received = jnp.concatenate(rows, axis=0)
        if members * FW > received.shape[1]:
            spare = jnp.zeros((2 * SP, FW), F32)
            for m in range(received.shape[1] // FW):
                part = roll(received[:, FW * m : FW * (m + 1)], 7 * m - 25)
                spare = jnp.where((fnode >= 7 * m) & (fnode < 7 * m + 7), part, spare)
            received = jnp.concatenate([received, spare], axis=1)
        got = own + right(hot_recv, received, 3)
        for a in range(2):
            for m in range(members):
                lanes = slice(FW * m, FW * (m + 1))
                lo = got[a * C : (a + 1) * C, lanes]
                hi = got[(2 + a) * C : (3 + a) * C, lanes]
                primal, tangent = swap(lo, hi)
                put(0, m, a, primal)
                put(1, m, a, tangent)

    def layer_outside(blocks, zr, members, put):
        for m in range(members):
            lanes = slice(FW * (m // 2), FW * (m // 2 + 1))
            step = 32 * (L - 1 if m % 2 == 0 else L - 2)
            lo = jnp.where(flayer == 0, roll(zr[0, :, lanes], -step), roll(blocks[2][m][1], 32))
            hi = jnp.where(flayer == L - 1, roll(zr[1, :, lanes], step), roll(blocks[2][m][0], -32))
            primal, tangent = swap(lo, hi)
            put(0, m, 2, primal)
            put(1, m, 2, tangent)

    whole = u[...].reshape(10 * C, VW)
    for a in range(3):
        faces = left(whole, pick_ref[a], 3).reshape(2, 5, C, FW)
        for m in range(5):
            uf[0, m, a] = faces[0, m] + fpad if m % 4 == 0 else faces[0, m]
            uf[1, m, a] = faces[1, m]
    blocks1, table1, sent1, zcopies1 = exchange(
        lambda pt, m, a: uf[pt, m, a], 5, sb1, rb1, zs1, zr1, 0
    )
    pcopies1 = finish_send(sent1, sb1, rb1, 0)
    pl.semaphore_wait(barrier, everyone - 1)
    for copy in pcopies1 + zcopies1:
        copy.start()
    for a in range(3):
        wide = jnp.zeros((C, VW), F32)
        face = jnp.zeros((C, FW), F32)
        for l in range(L):
            value = column(metric_ref[a, l : l + 1, :])
            wide = jnp.where(vl // 128 == l, value, wide)
            face = jnp.where(flayer == l, value, face)
        mv[a] = wide
        mf[a] = face

    for copy in inputs[7:]:
        copy.wait()

    own1 = sum(dot(hot_own, p) for p in table1[::-1])

    @pl.loop(0, C // 8, unroll=True)
    def _(i):
        rows = pl.ds(pl.multiple_of(i * 8, 8), 8)
        primal = [u[0, m, rows, :] for m in range(5)]
        tangent = [u[1, m, rows, :] for m in range(5)]
        fp, ft = jax.jvp(gradient_fields, (primal,), (tangent,))
        for m in range(4):
            w[0, m, rows, :] = fp[m]
            w[1, m, rows, :] = ft[m]

    fields = w[...].reshape(8 * C, VW)
    for a in range(3):
        q[a] = derive(fields, dh_ref[a], dl_ref[a]).reshape(2, 4, C, VW)

    for copy in zcopies1 + pcopies1:
        copy.wait()
    low_wall = jnp.where(source[2] < 0.0, 1.0, 0.0)
    high_wall = jnp.where(source[3] < 0.0, 1.0, 0.0)
    wall = jnp.where(first, low_wall, high_wall) > 0.5

    def put1(pt, m, a, value):
        if a == 1:
            own = uf[pt, m, a]
            value = jnp.where(wall, own if m % 4 == 0 else -own, value)
        of[pt, m, a] = jnp.where(fnode < 25, value, uf[pt, m, a])

    plane_outside(own1, rb1, 5, put1)
    layer_outside(blocks1, zr1, 5, put1)

    for a in range(3):
        @pl.loop(0, C // 8, unroll=True)
        def _(i):
            rows = pl.ds(pl.multiple_of(i * 8, 8), 8)
            primal = ([uf[0, m, a, rows, :] for m in range(5)], [of[0, m, a, rows, :] for m in range(5)])
            tangent = ([uf[1, m, a, rows, :] for m in range(5)], [of[1, m, a, rows, :] for m in range(5)])
            jp, jt = jax.jvp(jump_fields, primal, tangent)
            for m in range(4):
                jf[a, 0, m, rows, :] = (0.5 * LIFT) * sign * jp[m]
                jf[a, 1, m, rows, :] = (0.5 * LIFT) * sign * jt[m]

        q[a] += left(jf[a].reshape(8 * C, FW), lift_ref[a], 2).reshape(2, 4, C, VW)

    @pl.loop(0, C // 8, unroll=True)
    def _(i):
        rows = pl.ds(pl.multiple_of(i * 8, 8), 8)
        scale = [mv[a, rows, :] for a in range(3)]
        states = [[u[pt, m, rows, :] for m in range(5)] for pt in range(2)]
        grads = [
            [[scale[a] * q[a, pt, m, rows, :] for m in range(4)] for a in range(3)]
            for pt in range(2)
        ]
        vp, vt = jax.jvp(viscous_all, (states[0], grads[0]), (states[1], grads[1]))
        for a in range(3):
            for m in range(4):
                v[a, 0, m, rows, :] = vp[a][m]
                v[a, 1, m, rows, :] = vt[a][m]

    for a in range(3):
        vf[a] = left(v[a].reshape(8 * C, VW), pick_ref[a], 3).reshape(2, 4, C, FW)
    blocks2, table2, sent2, zcopies2 = exchange(
        lambda pt, m, a: vf[a, pt, m], 4, sb2, rb2, zs2, zr2, 4
    )
    pcopies2 = finish_send(sent2, sb2, rb2, 4)
    for copy in pcopies2 + zcopies2:
        copy.start()

    own2 = sum(dot(hot_own, p) for p in table2[::-1])

    @pl.loop(0, C // 8, unroll=True)
    def _(i):
        rows = pl.ds(pl.multiple_of(i * 8, 8), 8)
        states = [[u[pt, m, rows, :] for m in range(5)] for pt in range(2)]
        for a in range(3):
            scale = mv[a, rows, :]
            fluxes = jax.jvp(lambda x: inviscid(x, a), (states[0],), (states[1],))
            for pt in range(2):
                g[a, pt, 0, rows, :] = scale * fluxes[pt][0]
                for m in range(4):
                    g[a, pt, m + 1, rows, :] = scale * (fluxes[pt][m + 1] - v[a, pt, m, rows, :])

    for a in range(3):
        @pl.loop(0, C // 8, unroll=True)
        def _(i):
            rows = pl.ds(pl.multiple_of(i * 8, 8), 8)
            primal = ([uf[0, m, a, rows, :] for m in range(5)], [of[0, m, a, rows, :] for m in range(5)])
            tangent = ([uf[1, m, a, rows, :] for m in range(5)], [of[1, m, a, rows, :] for m in range(5)])
            sp, stt = jax.jvp(
                lambda inner, outer: surface(inner, outer, sign, a), primal, tangent
            )
            for m in range(5):
                s[a, 0, m, rows, :] = sp[m]
                s[a, 1, m, rows, :] = stt[m]

    total = None
    for a in range(3):
        part = derive(g[a].reshape(10 * C, VW), dh_ref[a], dl_ref[a])
        total = part if total is None else total + part
    r[...] = total.reshape(2, 5, C, VW)

    for copy in zcopies2 + pcopies2:
        copy.wait()

    def put2(pt, m, a, value):
        if a == 1:
            value = jnp.where(wall, vf[a, pt, m], value)
        ov[a, pt, m] = value

    plane_outside(own2, rb2, 4, put2)
    layer_outside(blocks2, zr2, 4, put2)
    lifted = None
    for a in range(3):
        for pt in range(2):
            s[a, pt, 0] = mf[a] * s[a, pt, 0]
            for m in range(4):
                jump = ov[a, pt, m] - vf[a, pt, m]
                s[a, pt, m + 1] = mf[a] * (s[a, pt, m + 1] - (0.5 * LIFT) * sign * jump)
        part = left(s[a].reshape(10 * C, FW), lift_ref[a], 2)
        lifted = part if lifted is None else lifted + part
    r[...] += lifted.reshape(2, 5, C, VW)

    def whole_sum(parts):
        acc = parts[0]
        for part in parts[1:]:
            acc = acc + part
        return jnp.sum(jnp.sum(acc, axis=0, keepdims=True), axis=1, keepdims=True)

    def ratio(top, bottom):
        return jnp.where(bottom > 0.0, top / jnp.where(bottom > 0.0, bottom, 1.0), 0.0)

    pd = whole_sum([r[1, m] * u[1, m] for m in range(5)])
    dd = whole_sum([u[1, m] * u[1, m] for m in range(5)])
    rs = whole_sum([r[0, m] * r[0, m] for m in range(5)])
    mine = ratio(pd, dd)
    rests = [r[1, m] - mine * u[1, m] for m in range(5)]
    rr = whole_sum([x * x for x in rests])
    rd = whole_sum([x * u[1, m] for m, x in enumerate(rests)])
    lane = lax.broadcasted_iota(jnp.int32, (1, 128), 1)
    row = jnp.zeros((1, 128), F32)
    for i, value in enumerate((pd, dd, rs, rr, rd)):
        row = jnp.where(lane == i, value, row)
    st[...] = row
    copies = [
        pltpu.make_async_remote_copy(
            src_ref=st, dst_ref=sta.at[k], send_sem=asend.at[k], recv_sem=arecv.at[k],
            device_id=peer(k), device_id_type=MESH,
        )
        for k in range(1, everyone)
    ]
    for copy in copies:
        copy.start()
    sta[0] = st[...]
    for l in range(L):
        for m in range(5):
            res_ref[:, l, 125 * m : 125 * (m + 1)] = r[0, m, :, 128 * l : 128 * l + 125]
    for copy in copies:
        copy.wait()
    table = sta[...].reshape(everyone, 128)
    pd, dd, rs, rr, rd = [
        jnp.sum(jnp.where(lane == i, table, 0.0), axis=1, keepdims=True) for i in range(5)
    ]
    coefficient = jnp.sum(pd, axis=0, keepdims=True) * (1.0 / total_count)
    shift = ratio(pd, dd) - coefficient
    rr = jnp.sum(rr + 2.0 * shift * rd + shift * shift * dd, axis=0, keepdims=True)
    rs = jnp.sum(rs, axis=0, keepdims=True)
    beta = jnp.sqrt(rr * (1.0 / total_count))
    norm = jnp.sqrt(rs * (1.0 / total_count))
    kry_ref[...] = jnp.where(lane == 0, coefficient, jnp.where(lane == 1, beta, norm))
    c, inv = coefficient, 1.0 / beta
    for m in range(5):
        value = (r[1, m] - c * u[1, m]) * inv
        for l in range(L):
            basis_ref[:, l, 125 * m : 125 * (m + 1)] = value[:, 128 * l : 128 * l + 125]


def local(ns, np_, state, direction, metric, face_source, send_rows):
    C, L, width = state.shape
    slots = send_rows.shape[2]
    SP = -(-slots // 8) * 8
    VW, FW = 128 * L, 64 * L
    own = 4 * C
    keys = np.full((1, own + 2 * SP), -7, np.int32)
    side, rest = np.divmod(np.arange(own), 2 * C)
    keys[0, :own] = 4 * (rest % C) + 2 * (rest // C) + side
    keys[0, own : own + slots] = own + np.arange(slots)
    keys[0, own + SP : own + SP + slots] = own + slots + np.arange(slots)
    tiles = 4 * (slots // 8) + -(-4 * (slots % 8) // 8)
    high, low, pick, lift = operators(L)
    operands = (
        state, direction, jnp.transpose(metric, (2, 1, 0)), face_source.T, send_rows,
        *[jnp.asarray(x) for x in (keys, high, low, pick, lift)],
    )
    vmem = lambda *shape: pltpu.VMEM(shape, F32)
    dma = lambda n: pltpu.SemaphoreType.DMA((n,))
    spec = pl.BlockSpec(memory_space=pltpu.VMEM)
    residual, basis, krylov = pl.pallas_call(
        functools.partial(kernel, ns, np_, float(state.size * ns * np_)),
        out_shape=(
            jax.ShapeDtypeStruct(state.shape, F32),
            jax.ShapeDtypeStruct(state.shape, F32),
            jax.ShapeDtypeStruct((1, 128), F32),
        ),
        in_specs=[pl.BlockSpec(memory_space=pltpu.HBM)] * 10,
        out_specs=(spec,) * 3,
        scratch_shapes=[
            vmem(2, 5, C, VW), vmem(2, 5, 3, C, FW), vmem(2, 5, 3, C, FW),
            vmem(2, 4, C, VW), vmem(3, 2, 4, C, FW), vmem(3, 2, 4, C, VW),
            vmem(3, 2, 4, C, VW), vmem(3, 2, 4, C, FW), vmem(3, 2, 4, C, FW),
            vmem(3, 2, 5, C, VW), vmem(3, 2, 5, C, FW), vmem(2, 5, C, VW),
            vmem(3, C, VW), vmem(3, C, FW),
            vmem(2, tiles, 8, FW), vmem(2, tiles, 8, FW), vmem(2, C, 3 * FW), vmem(2, C, 3 * FW),
            vmem(2, tiles, 8, FW), vmem(2, tiles, 8, FW), vmem(2, C, 2 * FW), vmem(2, C, 2 * FW),
            vmem(1, 128), vmem(ns * np_, 1, 128),
            *[pltpu.VMEM(x.shape, x.dtype) for x in operands],
            dma(8), dma(8), dma(ns * np_), dma(ns * np_), dma(10),
        ],
        compiler_params=pltpu.CompilerParams(
            collective_id=0, has_side_effects=True, vmem_limit_bytes=63 * 1024 * 1024
        ),
        name="navier",
    )(*operands)
    return residual, basis, krylov[0, :3]


def solution(mesh):
    return jax.shard_map(
        functools.partial(local, mesh.shape["stream"], mesh.shape["span"]),
        mesh=mesh,
        in_specs=(
            P("stream", "span", None),
            P("stream", "span", None),
            P("stream", "span", None),
            P("stream", None),
            P("stream", None, None),
        ),
        out_specs=(P("stream", "span", None), P("stream", "span", None), P()),
        check_vma=False,
    )
```

```python
import functools
import math

import jax
import jax.numpy as jnp
import numpy as np
from jax import lax
from jax.experimental import pallas as pl
from jax.experimental.pallas import tpu as pltpu
from jax.sharding import PartitionSpec as P

GAMMA = 1.4
VISC = 0.01
COND = VISC * GAMMA / ((GAMMA - 1.0) * 0.72)
LIFT = 10.0
MESH = pl.DeviceIdType.MESH
F32, BF16 = jnp.float32, jnp.bfloat16


def diff_table():
    spread = math.sqrt(3.0 / 7.0)
    points = np.array([-1.0, -spread, 0.0, spread, 1.0])
    weights = np.array(
        [np.prod([points[i] - points[j] for j in range(5) if j != i]) for i in range(5)]
    )
    matrix = np.zeros((5, 5))
    for i in range(5):
        for j in range(5):
            if i != j:
                matrix[i, j] = weights[i] / (weights[j] * (points[i] - points[j]))
        matrix[i, i] = np.sum([1.0 / (points[i] - points[j]) for j in range(5) if j != i])
    return matrix


def operators(layers):
    table = diff_table()
    eye = np.eye(5)
    kron = [
        np.einsum("ai,bj,ck->ijkabc", *[table if m == a else eye for m in range(3)]).reshape(125, 125)
        for a in range(3)
    ]
    node = np.arange(125).reshape(5, 5, 5)
    vw, fw, half = 128 * layers, 64 * layers, 32 * layers
    deriv = np.zeros((3, vw, vw), np.float32)
    pick = np.zeros((3, vw, fw), np.float32)
    for a in range(3):
        for l in range(layers):
            b = 128 * l
            deriv[a, b : b + 125, b : b + 125] = kron[a]
            for side in range(2):
                face = np.take(node, 4 * side, axis=a).reshape(-1)
                for m, at in enumerate(face):
                    pick[a, b + at, side * half + 32 * l + m] = 1.0
    high = deriv.astype(jnp.bfloat16)
    low = (deriv - high.astype(np.float32)).astype(jnp.bfloat16)
    lift = np.swapaxes(pick, 1, 2)
    return high, low, pick.astype(jnp.bfloat16), lift.astype(jnp.bfloat16)


def pieces(x, n):
    out = []
    for i in range(n):
        p = x.astype(BF16)
        out.append(p)
        if i + 1 < n:
            x = x - p.astype(F32)
    return out


def dot(a, b):
    return jnp.dot(a, b, preferred_element_type=F32)


def left(x, w, n):
    return sum(dot(p, w) for p in pieces(x, n)[::-1])


def right(w, x, n):
    return sum(dot(w, p) for p in pieces(x, n)[::-1])


def derive(x, high, low):
    a, b = pieces(x, 2)
    return dot(a, low) + dot(b, high) + dot(a, high)


def fields_of(u):
    inv = 1.0 / u[0]
    vel = [u[1] * inv, u[2] * inv, u[3] * inv]
    kinetic = 0.5 * (u[1] * vel[0] + u[2] * vel[1] + u[3] * vel[2])
    pressure = (GAMMA - 1.0) * (u[4] - kinetic)
    return vel, pressure, pressure * inv


def inviscid(u, a):
    vel, pressure, _ = fields_of(u)
    out = [u[1 + a]]
    for m in range(3):
        term = u[1 + m] * vel[a]
        out.append(term + pressure if m == a else term)
    out.append((u[4] + pressure) * vel[a])
    return out


def viscous(vel, q, a, divergence):
    stress = []
    for m in range(3):
        term = q[a][m] + q[m][a]
        if m == a:
            term = term - 2.0 / 3.0 * divergence
        stress.append(VISC * term)
    energy = stress[0] * vel[0] + stress[1] * vel[1] + stress[2] * vel[2] + COND * q[a][3]
    return stress + [energy]


def viscous_all(u, q):
    inv = 1.0 / u[0]
    vel = [u[1] * inv, u[2] * inv, u[3] * inv]
    divergence = q[0][0] + q[1][1] + q[2][2]
    return [viscous(vel, q, a, divergence) for a in range(3)]


def gradient_fields(u):
    vel, _, temper = fields_of(u)
    return vel + [temper]


def jump_fields(inner, outer):
    return [o - i for o, i in zip(gradient_fields(outer), gradient_fields(inner))]


def surface(inner, outer, sign, a):
    vi, pi, ti = fields_of(inner)
    vo, po, to = fields_of(outer)
    square = sum(v * v for v in vi) + GAMMA * ti + sum(v * v for v in vo) + GAMMA * to
    speed = jnp.sqrt(0.5 * square)
    fi, fo = inviscid(inner, a), inviscid(outer, a)
    return [
        (0.5 * LIFT) * (sign * (fo[m] - fi[m]) - speed * (outer[m] - inner[m])) for m in range(5)
    ]


def ratio(top, bottom):
    return jnp.where(bottom > 0.0, top / jnp.where(bottom > 0.0, bottom, 1.0), 0.0)


def kernel(
    ns, np_,
    x_hbm, d_hbm, metric_hbm, fs_hbm, sr_hbm, key_hbm, dh_hbm, dl_hbm, pick_hbm, lift_hbm,
    r_hbm, table_ref,
    u, uf, of, w, jf, q, v, vf, ov, g, s, r, mv, mf,
    sb1, rb1, zs1, zr1, sb2, rb2, zs2, zr2, st, sta,
    x_ref, d_ref, metric_ref, fs_ref, sr_ref, keyrow_ref, dh_ref, dl_ref, pick_ref, lift_ref,
    xsend, xrecv, asend, arecv, loads, store,
):
    C, L = x_ref.shape[0], x_ref.shape[1]
    VW, FW, half = 128 * L, 64 * L, 32 * L
    SLOTS = sr_ref.shape[2]
    SP = -(-SLOTS // 8) * 8
    MAIN, REM = SLOTS // 8, SLOTS % 8
    OWN = 4 * C
    ms, mp = lax.axis_index("stream"), lax.axis_index("span")
    lower, upper = lax.rem(ms + ns - 1, ns), lax.rem(ms + 1, ns)
    below, above = lax.rem(mp + np_ - 1, np_), lax.rem(mp + 1, np_)

    inputs = [
        pltpu.make_async_copy(src, dst, loads.at[i])
        for i, (src, dst) in enumerate(
            [
                (x_hbm, x_ref), (d_hbm, d_ref), (pick_hbm, pick_ref), (key_hbm, keyrow_ref),
                (fs_hbm, fs_ref), (sr_hbm, sr_ref), (metric_hbm, metric_ref),
                (dh_hbm, dh_ref), (dl_hbm, dl_ref), (lift_hbm, lift_ref),
            ]
        )
    ]
    for copy in inputs:
        copy.start()

    def peer(k):
        a, b = divmod(k, np_)
        return lax.rem(ms + a, ns), lax.rem(mp + b, np_)

    everyone = ns * np_
    barrier = pltpu.get_barrier_semaphore()
    for k in range(1, everyone):
        pl.semaphore_signal(barrier, inc=1, device_id=peer(k), device_id_type=MESH)

    fl = lax.broadcasted_iota(jnp.int32, (1, FW), 1)
    vl = lax.broadcasted_iota(jnp.int32, (1, VW), 1)
    first = fl < half
    sign = jnp.where(first, -1.0, 1.0)
    flayer = lax.rem(fl, half) // 32
    fnode = lax.rem(fl, 32)
    fpad = jnp.where(fnode >= 25, 1.0, 0.0)

    def roll(x, shift):
        shift = shift % FW
        return pltpu.roll(x, shift, 1) if shift else x

    di = lax.broadcasted_iota(jnp.int32, (C, C), 0)
    dj = lax.broadcasted_iota(jnp.int32, (C, C), 1)

    def column(row):
        return jnp.sum(jnp.where(di == dj, row, 0.0), axis=1, keepdims=True)

    for copy in inputs[:2]:
        copy.wait()

    for pt, ref in enumerate((x_ref, d_ref)):
        for l in range(L):
            for m in range(5):
                pad = 1.0 if pt == 0 and m % 4 == 0 else 0.0
                u[pt, m, :, 128 * l + 120 : 128 * (l + 1)] = jnp.full((C, 8), pad, F32)
                u[pt, m, :, 128 * l : 128 * l + 125] = ref[:, l, 125 * m : 125 * (m + 1)]
    for copy in inputs[2:7]:
        copy.wait()
    keyrow = keyrow_ref[...].astype(F32)
    source = [column(fs_ref[f : f + 1, :].astype(F32)) for f in range(4)]
    onehot = jnp.concatenate(
        [
            jnp.where(source[2 * a + side] == keyrow, 1.0, 0.0)
            for side in range(2)
            for a in range(2)
        ],
        axis=0,
    ).astype(BF16)
    hot_own, hot_recv = onehot[:, :OWN], onehot[:, OWN : OWN + 2 * SP]
    ri = lax.broadcasted_iota(jnp.int32, (SP, SLOTS), 0)
    li = lax.broadcasted_iota(jnp.int32, (SP, SLOTS), 1)
    send_hot = []
    for side in range(2):
        row = sr_ref[0, side : side + 1, :].astype(F32)
        wanted = jnp.sum(jnp.where(ri == li, row, 0.0), axis=1, keepdims=True)
        send_hot.append(jnp.where(wanted == keyrow[:, :OWN], 1.0, 0.0))
    send_hot = jnp.concatenate(send_hot, axis=0).astype(BF16)

    def swap(a, b):
        return (
            jnp.where(first, a, pltpu.roll(b, half, 1)),
            jnp.where(first, pltpu.roll(a, half, 1), b),
        )

    def exchange(faces, members, sb, rb, zs, zr, base):
        blocks = [[swap(faces(0, m, a), faces(1, m, a)) for m in range(members)] for a in range(3)]
        table = jnp.concatenate(
            [
                jnp.concatenate([blocks[a][m][side] for m in range(members)], axis=1)
                for side in range(2)
                for a in range(2)
            ],
            axis=0,
        )
        for m in range(0, members, 2):
            for side in range(2):
                value = blocks[2][m][side]
                if m + 1 < members:
                    other = roll(blocks[2][m + 1][side], 32 if side == 0 else -32)
                    value = jnp.where(flayer == (0 if side == 0 else L - 1), value, other)
                zs[side, :, FW * (m // 2) : FW * (m // 2 + 1)] = value
        zs_copies = [
            (zs.at[0], zr.at[1], (ms, below)),
            (zs.at[1], zr.at[0], (ms, above)),
        ]
        copies = []
        for i, (src, dst, to) in enumerate(zs_copies):
            copies.append(
                pltpu.make_async_remote_copy(
                    src_ref=src, dst_ref=dst, send_sem=xsend.at[base + i],
                    recv_sem=xrecv.at[base + i], device_id=to, device_id_type=MESH,
                )
            )
        table_pieces = pieces(table, 3)
        sent = sum(dot(send_hot, p) for p in table_pieces[::-1])
        return blocks, table_pieces, sent, copies

    def finish_send(sent, sb, rb, base):
        for m in range(4):
            value = sent[:, FW * m : FW * (m + 1)]
            if sent.shape[1] > 4 * FW:
                spare = roll(sent[:, 4 * FW :], 25 - 7 * m)
                value = jnp.where(fnode < 25, value, spare)
            for side in range(2):
                for b in range(MAIN):
                    at = side * SP + 8 * b
                    sb[side, 4 * b + m] = value[at : at + 8]
                for e in range(REM):
                    at, to = side * SP + 8 * MAIN + e, REM * m + e
                    sb[side, 4 * MAIN + to // 8, to % 8 : to % 8 + 1, :] = value[at : at + 1]
        out = []
        for i, (src, dst, to) in enumerate(
            [
                (sb.at[0], rb.at[1], (lower, mp)),
                (sb.at[1], rb.at[0], (upper, mp)),
            ]
        ):
            out.append(
                pltpu.make_async_remote_copy(
                    src_ref=src, dst_ref=dst, send_sem=xsend.at[base + 2 + i],
                    recv_sem=xrecv.at[base + 2 + i], device_id=to, device_id_type=MESH,
                )
            )
        return out

    def plane_outside(own, rb, members, put):
        row8 = lax.broadcasted_iota(jnp.int32, (8, 1), 0)
        rows = []
        for side in range(2):
            rows += [
                jnp.concatenate([rb[side, 4 * b + m] for m in range(4)], axis=1)
                for b in range(MAIN)
            ]
            if REM:
                parts = []
                for m in range(4):
                    part = jnp.zeros((8, FW), F32)
                    for e in range(REM):
                        to = REM * m + e
                        line = rb[side, 4 * MAIN + to // 8, to % 8 : to % 8 + 1, :]
                        part = jnp.where(row8 == e, line, part)
                    parts.append(part)
                rows.append(jnp.concatenate(parts, axis=1))
        received = jnp.concatenate(rows, axis=0)
        if members * FW > received.shape[1]:
            spare = jnp.zeros((2 * SP, FW), F32)
            for m in range(received.shape[1] // FW):
                part = roll(received[:, FW * m : FW * (m + 1)], 7 * m - 25)
                spare = jnp.where((fnode >= 7 * m) & (fnode < 7 * m + 7), part, spare)
            received = jnp.concatenate([received, spare], axis=1)
        got = own + right(hot_recv, received, 3)
        for a in range(2):
            for m in range(members):
                lanes = slice(FW * m, FW * (m + 1))
                lo = got[a * C : (a + 1) * C, lanes]
                hi = got[(2 + a) * C : (3 + a) * C, lanes]
                primal, tangent = swap(lo, hi)
                put(0, m, a, primal)
                put(1, m, a, tangent)

    def layer_outside(blocks, zr, members, put):
        for m in range(members):
            lanes = slice(FW * (m // 2), FW * (m // 2 + 1))
            step = 32 * (L - 1 if m % 2 == 0 else L - 2)
            lo = jnp.where(flayer == 0, roll(zr[0, :, lanes], -step), roll(blocks[2][m][1], 32))
            hi = jnp.where(flayer == L - 1, roll(zr[1, :, lanes], step), roll(blocks[2][m][0], -32))
            primal, tangent = swap(lo, hi)
            put(0, m, 2, primal)
            put(1, m, 2, tangent)

    whole = u[...].reshape(10 * C, VW)
    for a in range(3):
        faces = left(whole, pick_ref[a], 3).reshape(2, 5, C, FW)
        for m in range(5):
            uf[0, m, a] = faces[0, m] + fpad if m % 4 == 0 else faces[0, m]
            uf[1, m, a] = faces[1, m]
    blocks1, table1, sent1, zcopies1 = exchange(
        lambda pt, m, a: uf[pt, m, a], 5, sb1, rb1, zs1, zr1, 0
    )
    pcopies1 = finish_send(sent1, sb1, rb1, 0)
    pl.semaphore_wait(barrier, everyone - 1)
    for copy in pcopies1 + zcopies1:
        copy.start()
    for a in range(3):
        wide = jnp.zeros((C, VW), F32)
        face = jnp.zeros((C, FW), F32)
        for l in range(L):
            value = column(metric_ref[a, l : l + 1, :])
            wide = jnp.where(vl // 128 == l, value, wide)
            face = jnp.where(flayer == l, value, face)
        mv[a] = wide
        mf[a] = face

    for copy in inputs[7:]:
        copy.wait()

    own1 = sum(dot(hot_own, p) for p in table1[::-1])

    @pl.loop(0, C // 8, unroll=True)
    def _(i):
        rows = pl.ds(pl.multiple_of(i * 8, 8), 8)
        primal = [u[0, m, rows, :] for m in range(5)]
        tangent = [u[1, m, rows, :] for m in range(5)]
        fp, ft = jax.jvp(gradient_fields, (primal,), (tangent,))
        for m in range(4):
            w[0, m, rows, :] = fp[m]
            w[1, m, rows, :] = ft[m]

    fields = w[...].reshape(8 * C, VW)
    for a in range(3):
        q[a] = derive(fields, dh_ref[a], dl_ref[a]).reshape(2, 4, C, VW)

    for copy in zcopies1 + pcopies1:
        copy.wait()
    low_wall = jnp.where(source[2] < 0.0, 1.0, 0.0)
    high_wall = jnp.where(source[3] < 0.0, 1.0, 0.0)
    wall = jnp.where(first, low_wall, high_wall) > 0.5

    def put1(pt, m, a, value):
        if a == 1:
            own = uf[pt, m, a]
            value = jnp.where(wall, own if m % 4 == 0 else -own, value)
        of[pt, m, a] = jnp.where(fnode < 25, value, uf[pt, m, a])

    plane_outside(own1, rb1, 5, put1)
    layer_outside(blocks1, zr1, 5, put1)

    for a in range(3):
        @pl.loop(0, C // 8, unroll=True)
        def _(i):
            rows = pl.ds(pl.multiple_of(i * 8, 8), 8)
            primal = ([uf[0, m, a, rows, :] for m in range(5)], [of[0, m, a, rows, :] for m in range(5)])
            tangent = ([uf[1, m, a, rows, :] for m in range(5)], [of[1, m, a, rows, :] for m in range(5)])
            jp, jt = jax.jvp(jump_fields, primal, tangent)
            for m in range(4):
                jf[a, 0, m, rows, :] = (0.5 * LIFT) * sign * jp[m]
                jf[a, 1, m, rows, :] = (0.5 * LIFT) * sign * jt[m]

        q[a] += left(jf[a].reshape(8 * C, FW), lift_ref[a], 2).reshape(2, 4, C, VW)

    @pl.loop(0, C // 8, unroll=True)
    def _(i):
        rows = pl.ds(pl.multiple_of(i * 8, 8), 8)
        scale = [mv[a, rows, :] for a in range(3)]
        states = [[u[pt, m, rows, :] for m in range(5)] for pt in range(2)]
        grads = [
            [[scale[a] * q[a, pt, m, rows, :] for m in range(4)] for a in range(3)]
            for pt in range(2)
        ]
        vp, vt = jax.jvp(viscous_all, (states[0], grads[0]), (states[1], grads[1]))
        for a in range(3):
            for m in range(4):
                v[a, 0, m, rows, :] = vp[a][m]
                v[a, 1, m, rows, :] = vt[a][m]

    for a in range(3):
        vf[a] = left(v[a].reshape(8 * C, VW), pick_ref[a], 3).reshape(2, 4, C, FW)
    blocks2, table2, sent2, zcopies2 = exchange(
        lambda pt, m, a: vf[a, pt, m], 4, sb2, rb2, zs2, zr2, 4
    )
    pcopies2 = finish_send(sent2, sb2, rb2, 4)
    for copy in pcopies2 + zcopies2:
        copy.start()

    own2 = sum(dot(hot_own, p) for p in table2[::-1])

    @pl.loop(0, C // 8, unroll=True)
    def _(i):
        rows = pl.ds(pl.multiple_of(i * 8, 8), 8)
        states = [[u[pt, m, rows, :] for m in range(5)] for pt in range(2)]
        for a in range(3):
            scale = mv[a, rows, :]
            fluxes = jax.jvp(lambda x: inviscid(x, a), (states[0],), (states[1],))
            for pt in range(2):
                g[a, pt, 0, rows, :] = scale * fluxes[pt][0]
                for m in range(4):
                    g[a, pt, m + 1, rows, :] = scale * (fluxes[pt][m + 1] - v[a, pt, m, rows, :])

    for a in range(3):
        @pl.loop(0, C // 8, unroll=True)
        def _(i):
            rows = pl.ds(pl.multiple_of(i * 8, 8), 8)
            primal = ([uf[0, m, a, rows, :] for m in range(5)], [of[0, m, a, rows, :] for m in range(5)])
            tangent = ([uf[1, m, a, rows, :] for m in range(5)], [of[1, m, a, rows, :] for m in range(5)])
            sp, stt = jax.jvp(
                lambda inner, outer: surface(inner, outer, sign, a), primal, tangent
            )
            for m in range(5):
                s[a, 0, m, rows, :] = sp[m]
                s[a, 1, m, rows, :] = stt[m]

    total = None
    for a in range(3):
        part = derive(g[a].reshape(10 * C, VW), dh_ref[a], dl_ref[a])
        total = part if total is None else total + part
    r[...] = total.reshape(2, 5, C, VW)

    for copy in zcopies2 + pcopies2:
        copy.wait()

    def put2(pt, m, a, value):
        if a == 1:
            value = jnp.where(wall, vf[a, pt, m], value)
        ov[a, pt, m] = value

    plane_outside(own2, rb2, 4, put2)
    layer_outside(blocks2, zr2, 4, put2)
    lifted = None
    for a in range(3):
        for pt in range(2):
            s[a, pt, 0] = mf[a] * s[a, pt, 0]
            for m in range(4):
                jump = ov[a, pt, m] - vf[a, pt, m]
                s[a, pt, m + 1] = mf[a] * (s[a, pt, m + 1] - (0.5 * LIFT) * sign * jump)
        part = left(s[a].reshape(10 * C, FW), lift_ref[a], 2)
        lifted = part if lifted is None else lifted + part
    r[...] += lifted.reshape(2, 5, C, VW)

    writing = pltpu.make_async_copy(r, r_hbm, store.at[0])
    writing.start()

    def whole_sum(parts):
        acc = parts[0]
        for part in parts[1:]:
            acc = acc + part
        return jnp.sum(jnp.sum(acc, axis=0, keepdims=True), axis=1, keepdims=True)

    pd = whole_sum([r[1, m] * u[1, m] for m in range(5)])
    dd = whole_sum([u[1, m] * u[1, m] for m in range(5)])
    rs = whole_sum([r[0, m] * r[0, m] for m in range(5)])
    mine = ratio(pd, dd)
    rests = [r[1, m] - mine * u[1, m] for m in range(5)]
    rr = whole_sum([x * x for x in rests])
    rd = whole_sum([x * u[1, m] for m, x in enumerate(rests)])
    lane = lax.broadcasted_iota(jnp.int32, (1, 128), 1)
    row = jnp.zeros((1, 128), F32)
    for i, value in enumerate((pd, dd, rs, rr, rd)):
        row = jnp.where(lane == i, value, row)
    st[...] = row
    copies = [
        pltpu.make_async_remote_copy(
            src_ref=st, dst_ref=sta.at[k], send_sem=asend.at[k], recv_sem=arecv.at[k],
            device_id=peer(k), device_id_type=MESH,
        )
        for k in range(1, everyone)
    ]
    for copy in copies:
        copy.start()
    sta[0] = st[...]
    for copy in copies:
        copy.wait()
    table_ref[...] = sta[...].reshape(everyone, 128)
    writing.wait()


def finish(
    total_count, r_hbm, d_hbm, table_hbm, res_hbm, basis_hbm, kry_ref, r, d, table_ref, res, basis, sems
):
    C, L = d.shape[0], d.shape[1]
    loads = [
        pltpu.make_async_copy(src, dst, sems.at[i])
        for i, (src, dst) in enumerate([(r_hbm, r), (d_hbm, d), (table_hbm, table_ref)])
    ]
    for copy in loads:
        copy.start()
    loads[0].wait()
    for l in range(L):
        for m in range(5):
            res[:, l, 125 * m : 125 * (m + 1)] = r[0, m, :, 128 * l : 128 * l + 125]
    first = pltpu.make_async_copy(res, res_hbm, sems.at[3])
    first.start()
    for copy in loads[1:]:
        copy.wait()
    lane = lax.broadcasted_iota(jnp.int32, (1, 128), 1)
    table = table_ref[...]
    pd, dd, rs, rr, rd = [
        jnp.sum(jnp.where(lane == i, table, 0.0), axis=1, keepdims=True) for i in range(5)
    ]
    coefficient = jnp.sum(pd, axis=0, keepdims=True) * (1.0 / total_count)
    shift = ratio(pd, dd) - coefficient
    rr = jnp.sum(rr + 2.0 * shift * rd + shift * shift * dd, axis=0, keepdims=True)
    rs = jnp.sum(rs, axis=0, keepdims=True)
    beta = jnp.sqrt(rr * (1.0 / total_count))
    norm = jnp.sqrt(rs * (1.0 / total_count))
    row = jnp.where(lane == 0, coefficient, jnp.where(lane == 1, beta, norm))
    kry_ref[...] = row[0, :3]
    c, inv = coefficient, 1.0 / beta
    for l in range(L):
        for m in range(5):
            at = slice(125 * m, 125 * (m + 1))
            product = r[1, m, :, 128 * l : 128 * l + 125]
            basis[:, l, at] = (product - c * d[:, l, at]) * inv
    second = pltpu.make_async_copy(basis, basis_hbm, sems.at[4])
    second.start()
    first.wait()
    second.wait()


def local(ns, np_, state, direction, metric, face_source, send_rows):
    C, L, width = state.shape
    slots = send_rows.shape[2]
    SP = -(-slots // 8) * 8
    VW, FW = 128 * L, 64 * L
    own = 4 * C
    keys = np.full((1, own + 2 * SP), -7, np.int32)
    side, rest = np.divmod(np.arange(own), 2 * C)
    keys[0, :own] = 4 * (rest % C) + 2 * (rest // C) + side
    keys[0, own : own + slots] = own + np.arange(slots)
    keys[0, own + SP : own + SP + slots] = own + slots + np.arange(slots)
    tiles = 4 * (slots // 8) + -(-4 * (slots % 8) // 8)
    high, low, pick, lift = operators(L)
    operands = (
        state, direction, jnp.transpose(metric, (2, 1, 0)), face_source.T, send_rows,
        *[jnp.asarray(x) for x in (keys, high, low, pick, lift)],
    )
    vmem = lambda *shape: pltpu.VMEM(shape, F32)
    dma = lambda n: pltpu.SemaphoreType.DMA((n,))
    spec = pl.BlockSpec(memory_space=pltpu.VMEM)
    parts, table = pl.pallas_call(
        functools.partial(kernel, ns, np_),
        out_shape=(
            jax.ShapeDtypeStruct((2, 5, C, VW), F32),
            jax.ShapeDtypeStruct((ns * np_, 128), F32),
        ),
        in_specs=[pl.BlockSpec(memory_space=pltpu.HBM)] * 10,
        out_specs=(pl.BlockSpec(memory_space=pltpu.HBM), spec),
        scratch_shapes=[
            vmem(2, 5, C, VW), vmem(2, 5, 3, C, FW), vmem(2, 5, 3, C, FW),
            vmem(2, 4, C, VW), vmem(3, 2, 4, C, FW), vmem(3, 2, 4, C, VW),
            vmem(3, 2, 4, C, VW), vmem(3, 2, 4, C, FW), vmem(3, 2, 4, C, FW),
            vmem(3, 2, 5, C, VW), vmem(3, 2, 5, C, FW), vmem(2, 5, C, VW),
            vmem(3, C, VW), vmem(3, C, FW),
            vmem(2, tiles, 8, FW), vmem(2, tiles, 8, FW), vmem(2, C, 3 * FW), vmem(2, C, 3 * FW),
            vmem(2, tiles, 8, FW), vmem(2, tiles, 8, FW), vmem(2, C, 2 * FW), vmem(2, C, 2 * FW),
            vmem(1, 128), vmem(ns * np_, 1, 128),
            *[pltpu.VMEM(x.shape, x.dtype) for x in operands],
            dma(8), dma(8), dma(ns * np_), dma(ns * np_), dma(10), dma(1),
        ],
        compiler_params=pltpu.CompilerParams(
            collective_id=0, has_side_effects=True, vmem_limit_bytes=63 * 1024 * 1024
        ),
        name="navier",
    )(*operands)
    hbm = pl.BlockSpec(memory_space=pltpu.HBM)
    return pl.pallas_call(
        functools.partial(finish, float(state.size * ns * np_)),
        out_shape=(
            jax.ShapeDtypeStruct(state.shape, F32),
            jax.ShapeDtypeStruct(state.shape, F32),
            jax.ShapeDtypeStruct((3,), F32),
        ),
        in_specs=[hbm] * 3,
        out_specs=(hbm, hbm, spec),
        scratch_shapes=[
            vmem(2, 5, C, VW), vmem(C, L, width), vmem(ns * np_, 128),
            vmem(C, L, width), vmem(C, L, width), dma(5),
        ],
        compiler_params=pltpu.CompilerParams(vmem_limit_bytes=63 * 1024 * 1024),
        name="finish",
    )(parts, direction, table)


def solution(mesh):
    return jax.shard_map(
        functools.partial(local, mesh.shape["stream"], mesh.shape["span"]),
        mesh=mesh,
        in_specs=(
            P("stream", "span", None),
            P("stream", "span", None),
            P("stream", "span", None),
            P("stream", None),
            P("stream", None, None),
        ),
        out_specs=(P("stream", "span", None), P("stream", "span", None), P()),
        check_vma=False,
    )
```

```python
import functools
import math

import jax
import jax.numpy as jnp
import numpy as np
from jax import lax
from jax.experimental import pallas as pl
from jax.experimental.pallas import tpu as pltpu
from jax.sharding import PartitionSpec as P

GAMMA = 1.4
VISC = 0.01
COND = VISC * GAMMA / ((GAMMA - 1.0) * 0.72)
LIFT = 10.0
MESH = pl.DeviceIdType.MESH
F32, BF16 = jnp.float32, jnp.bfloat16


def diff_table():
    spread = math.sqrt(3.0 / 7.0)
    points = np.array([-1.0, -spread, 0.0, spread, 1.0])
    weights = np.array(
        [np.prod([points[i] - points[j] for j in range(5) if j != i]) for i in range(5)]
    )
    matrix = np.zeros((5, 5))
    for i in range(5):
        for j in range(5):
            if i != j:
                matrix[i, j] = weights[i] / (weights[j] * (points[i] - points[j]))
        matrix[i, i] = np.sum([1.0 / (points[i] - points[j]) for j in range(5) if j != i])
    return matrix


def operators(layers):
    table = diff_table()
    eye = np.eye(5)
    kron = [
        np.einsum("ai,bj,ck->ijkabc", *[table if m == a else eye for m in range(3)]).reshape(125, 125)
        for a in range(3)
    ]
    node = np.arange(125).reshape(5, 5, 5)
    vw, fw, half = 128 * layers, 64 * layers, 32 * layers
    deriv = np.zeros((3, vw, vw), np.float32)
    pick = np.zeros((3, vw, fw), np.float32)
    for a in range(3):
        for l in range(layers):
            b = 128 * l
            deriv[a, b : b + 125, b : b + 125] = kron[a]
            for side in range(2):
                face = np.take(node, 4 * side, axis=a).reshape(-1)
                for m, at in enumerate(face):
                    pick[a, b + at, side * half + 32 * l + m] = 1.0
    high = deriv.astype(jnp.bfloat16)
    low = (deriv - high.astype(np.float32)).astype(jnp.bfloat16)
    lift = np.swapaxes(pick, 1, 2)
    return high, low, pick.astype(jnp.bfloat16), lift.astype(jnp.bfloat16)


def pieces(x, n):
    out = []
    for i in range(n):
        p = x.astype(BF16)
        out.append(p)
        if i + 1 < n:
            x = x - p.astype(F32)
    return out


def dot(a, b):
    return jnp.dot(a, b, preferred_element_type=F32)


def left(x, w, n):
    return sum(dot(p, w) for p in pieces(x, n)[::-1])


def right(w, x, n):
    return sum(dot(w, p) for p in pieces(x, n)[::-1])


def derive(x, high, low):
    a, b = pieces(x, 2)
    return dot(a, low) + dot(b, high) + dot(a, high)


def fields_of(u):
    inv = 1.0 / u[0]
    vel = [u[1] * inv, u[2] * inv, u[3] * inv]
    kinetic = 0.5 * (u[1] * vel[0] + u[2] * vel[1] + u[3] * vel[2])
    pressure = (GAMMA - 1.0) * (u[4] - kinetic)
    return vel, pressure, pressure * inv


def inviscid(u, a):
    vel, pressure, _ = fields_of(u)
    out = [u[1 + a]]
    for m in range(3):
        term = u[1 + m] * vel[a]
        out.append(term + pressure if m == a else term)
    out.append((u[4] + pressure) * vel[a])
    return out


def viscous(vel, q, a, divergence):
    stress = []
    for m in range(3):
        term = q[a][m] + q[m][a]
        if m == a:
            term = term - 2.0 / 3.0 * divergence
        stress.append(VISC * term)
    energy = stress[0] * vel[0] + stress[1] * vel[1] + stress[2] * vel[2] + COND * q[a][3]
    return stress + [energy]


def viscous_all(u, q):
    inv = 1.0 / u[0]
    vel = [u[1] * inv, u[2] * inv, u[3] * inv]
    divergence = q[0][0] + q[1][1] + q[2][2]
    return [viscous(vel, q, a, divergence) for a in range(3)]


def gradient_fields(u):
    vel, _, temper = fields_of(u)
    return vel + [temper]


def jump_fields(inner, outer):
    return [o - i for o, i in zip(gradient_fields(outer), gradient_fields(inner))]


def surface(inner, outer, sign, a):
    vi, pi, ti = fields_of(inner)
    vo, po, to = fields_of(outer)
    square = sum(v * v for v in vi) + GAMMA * ti + sum(v * v for v in vo) + GAMMA * to
    speed = jnp.sqrt(0.5 * square)
    fi, fo = inviscid(inner, a), inviscid(outer, a)
    return [
        (0.5 * LIFT) * (sign * (fo[m] - fi[m]) - speed * (outer[m] - inner[m])) for m in range(5)
    ]


def ratio(top, bottom):
    return jnp.where(bottom > 0.0, top / jnp.where(bottom > 0.0, bottom, 1.0), 0.0)


def kernel(
    ns, np_,
    x_hbm, d_hbm, metric_hbm, fs_hbm, sr_hbm, key_hbm, dh_hbm, dl_hbm, pick_hbm, lift_hbm,
    res_hbm, prod_hbm, table_ref,
    u, uf, of, w, jf, q, v, vf, ov, g, s, r, mv, mf,
    sb1, rb1, zs1, zr1, sb2, rb2, zs2, zr2, st, sta,
    x_ref, d_ref, metric_ref, fs_ref, sr_ref, keyrow_ref, dh_ref, dl_ref, pick_ref, lift_ref,
    xsend, xrecv, asend, arecv, loads, store, res, prod,
):
    C, L = x_ref.shape[0], x_ref.shape[1]
    VW, FW, half = 128 * L, 64 * L, 32 * L
    SLOTS = sr_ref.shape[2]
    SP = -(-SLOTS // 8) * 8
    MAIN, REM = SLOTS // 8, SLOTS % 8
    OWN = 4 * C
    ms, mp = lax.axis_index("stream"), lax.axis_index("span")
    lower, upper = lax.rem(ms + ns - 1, ns), lax.rem(ms + 1, ns)
    below, above = lax.rem(mp + np_ - 1, np_), lax.rem(mp + 1, np_)

    inputs = [
        pltpu.make_async_copy(src, dst, loads.at[i])
        for i, (src, dst) in enumerate(
            [
                (x_hbm, x_ref), (d_hbm, d_ref), (pick_hbm, pick_ref), (key_hbm, keyrow_ref),
                (fs_hbm, fs_ref), (sr_hbm, sr_ref), (metric_hbm, metric_ref),
                (dh_hbm, dh_ref), (dl_hbm, dl_ref), (lift_hbm, lift_ref),
            ]
        )
    ]
    for copy in inputs:
        copy.start()

    def peer(k):
        a, b = divmod(k, np_)
        return lax.rem(ms + a, ns), lax.rem(mp + b, np_)

    everyone = ns * np_
    barrier = pltpu.get_barrier_semaphore()
    for k in range(1, everyone):
        pl.semaphore_signal(barrier, inc=1, device_id=peer(k), device_id_type=MESH)

    fl = lax.broadcasted_iota(jnp.int32, (1, FW), 1)
    vl = lax.broadcasted_iota(jnp.int32, (1, VW), 1)
    first = fl < half
    sign = jnp.where(first, -1.0, 1.0)
    flayer = lax.rem(fl, half) // 32
    fnode = lax.rem(fl, 32)
    fpad = jnp.where(fnode >= 25, 1.0, 0.0)

    def roll(x, shift):
        shift = shift % FW
        return pltpu.roll(x, shift, 1) if shift else x

    di = lax.broadcasted_iota(jnp.int32, (C, C), 0)
    dj = lax.broadcasted_iota(jnp.int32, (C, C), 1)

    def column(row):
        return jnp.sum(jnp.where(di == dj, row, 0.0), axis=1, keepdims=True)

    for copy in inputs[:2]:
        copy.wait()

    for pt, ref in enumerate((x_ref, d_ref)):
        for l in range(L):
            for m in range(5):
                pad = 1.0 if pt == 0 and m % 4 == 0 else 0.0
                u[pt, m, :, 128 * l + 120 : 128 * (l + 1)] = jnp.full((C, 8), pad, F32)
                u[pt, m, :, 128 * l : 128 * l + 125] = ref[:, l, 125 * m : 125 * (m + 1)]
    for copy in inputs[2:7]:
        copy.wait()
    keyrow = keyrow_ref[...].astype(F32)
    source = [column(fs_ref[f : f + 1, :].astype(F32)) for f in range(4)]
    onehot = jnp.concatenate(
        [
            jnp.where(source[2 * a + side] == keyrow, 1.0, 0.0)
            for side in range(2)
            for a in range(2)
        ],
        axis=0,
    ).astype(BF16)
    hot_own, hot_recv = onehot[:, :OWN], onehot[:, OWN : OWN + 2 * SP]
    ri = lax.broadcasted_iota(jnp.int32, (SP, SLOTS), 0)
    li = lax.broadcasted_iota(jnp.int32, (SP, SLOTS), 1)
    send_hot = []
    for side in range(2):
        row = sr_ref[0, side : side + 1, :].astype(F32)
        wanted = jnp.sum(jnp.where(ri == li, row, 0.0), axis=1, keepdims=True)
        send_hot.append(jnp.where(wanted == keyrow[:, :OWN], 1.0, 0.0))
    send_hot = jnp.concatenate(send_hot, axis=0).astype(BF16)

    def swap(a, b):
        return (
            jnp.where(first, a, pltpu.roll(b, half, 1)),
            jnp.where(first, pltpu.roll(a, half, 1), b),
        )

    def exchange(faces, members, sb, rb, zs, zr, base):
        blocks = [[swap(faces(0, m, a), faces(1, m, a)) for m in range(members)] for a in range(3)]
        table = jnp.concatenate(
            [
                jnp.concatenate([blocks[a][m][side] for m in range(members)], axis=1)
                for side in range(2)
                for a in range(2)
            ],
            axis=0,
        )
        for m in range(0, members, 2):
            for side in range(2):
                value = blocks[2][m][side]
                if m + 1 < members:
                    other = roll(blocks[2][m + 1][side], 32 if side == 0 else -32)
                    value = jnp.where(flayer == (0 if side == 0 else L - 1), value, other)
                zs[side, :, FW * (m // 2) : FW * (m // 2 + 1)] = value
        zs_copies = [
            (zs.at[0], zr.at[1], (ms, below)),
            (zs.at[1], zr.at[0], (ms, above)),
        ]
        copies = []
        for i, (src, dst, to) in enumerate(zs_copies):
            copies.append(
                pltpu.make_async_remote_copy(
                    src_ref=src, dst_ref=dst, send_sem=xsend.at[base + i],
                    recv_sem=xrecv.at[base + i], device_id=to, device_id_type=MESH,
                )
            )
        table_pieces = pieces(table, 3)
        sent = sum(dot(send_hot, p) for p in table_pieces[::-1])
        return blocks, table_pieces, sent, copies

    def finish_send(sent, sb, rb, base):
        for m in range(4):
            value = sent[:, FW * m : FW * (m + 1)]
            if sent.shape[1] > 4 * FW:
                spare = roll(sent[:, 4 * FW :], 25 - 7 * m)
                value = jnp.where(fnode < 25, value, spare)
            for side in range(2):
                for b in range(MAIN):
                    at = side * SP + 8 * b
                    sb[side, 4 * b + m] = value[at : at + 8]
                for e in range(REM):
                    at, to = side * SP + 8 * MAIN + e, REM * m + e
                    sb[side, 4 * MAIN + to // 8, to % 8 : to % 8 + 1, :] = value[at : at + 1]
        out = []
        for i, (src, dst, to) in enumerate(
            [
                (sb.at[0], rb.at[1], (lower, mp)),
                (sb.at[1], rb.at[0], (upper, mp)),
            ]
        ):
            out.append(
                pltpu.make_async_remote_copy(
                    src_ref=src, dst_ref=dst, send_sem=xsend.at[base + 2 + i],
                    recv_sem=xrecv.at[base + 2 + i], device_id=to, device_id_type=MESH,
                )
            )
        return out

    def plane_outside(own, rb, members, put):
        row8 = lax.broadcasted_iota(jnp.int32, (8, 1), 0)
        rows = []
        for side in range(2):
            rows += [
                jnp.concatenate([rb[side, 4 * b + m] for m in range(4)], axis=1)
                for b in range(MAIN)
            ]
            if REM:
                parts = []
                for m in range(4):
                    part = jnp.zeros((8, FW), F32)
                    for e in range(REM):
                        to = REM * m + e
                        line = rb[side, 4 * MAIN + to // 8, to % 8 : to % 8 + 1, :]
                        part = jnp.where(row8 == e, line, part)
                    parts.append(part)
                rows.append(jnp.concatenate(parts, axis=1))
        received = jnp.concatenate(rows, axis=0)
        if members * FW > received.shape[1]:
            spare = jnp.zeros((2 * SP, FW), F32)
            for m in range(received.shape[1] // FW):
                part = roll(received[:, FW * m : FW * (m + 1)], 7 * m - 25)
                spare = jnp.where((fnode >= 7 * m) & (fnode < 7 * m + 7), part, spare)
            received = jnp.concatenate([received, spare], axis=1)
        got = own + right(hot_recv, received, 3)
        for a in range(2):
            for m in range(members):
                lanes = slice(FW * m, FW * (m + 1))
                lo = got[a * C : (a + 1) * C, lanes]
                hi = got[(2 + a) * C : (3 + a) * C, lanes]
                primal, tangent = swap(lo, hi)
                put(0, m, a, primal)
                put(1, m, a, tangent)

    def layer_outside(blocks, zr, members, put):
        for m in range(members):
            lanes = slice(FW * (m // 2), FW * (m // 2 + 1))
            step = 32 * (L - 1 if m % 2 == 0 else L - 2)
            lo = jnp.where(flayer == 0, roll(zr[0, :, lanes], -step), roll(blocks[2][m][1], 32))
            hi = jnp.where(flayer == L - 1, roll(zr[1, :, lanes], step), roll(blocks[2][m][0], -32))
            primal, tangent = swap(lo, hi)
            put(0, m, 2, primal)
            put(1, m, 2, tangent)

    whole = u[...].reshape(10 * C, VW)
    for a in range(3):
        faces = left(whole, pick_ref[a], 3).reshape(2, 5, C, FW)
        for m in range(5):
            uf[0, m, a] = faces[0, m] + fpad if m % 4 == 0 else faces[0, m]
            uf[1, m, a] = faces[1, m]
    blocks1, table1, sent1, zcopies1 = exchange(
        lambda pt, m, a: uf[pt, m, a], 5, sb1, rb1, zs1, zr1, 0
    )
    pcopies1 = finish_send(sent1, sb1, rb1, 0)
    pl.semaphore_wait(barrier, everyone - 1)
    for copy in pcopies1 + zcopies1:
        copy.start()
    for a in range(3):
        wide = jnp.zeros((C, VW), F32)
        face = jnp.zeros((C, FW), F32)
        for l in range(L):
            value = column(metric_ref[a, l : l + 1, :])
            wide = jnp.where(vl // 128 == l, value, wide)
            face = jnp.where(flayer == l, value, face)
        mv[a] = wide
        mf[a] = face

    for copy in inputs[7:]:
        copy.wait()

    own1 = sum(dot(hot_own, p) for p in table1[::-1])

    @pl.loop(0, C // 8, unroll=True)
    def _(i):
        rows = pl.ds(pl.multiple_of(i * 8, 8), 8)
        primal = [u[0, m, rows, :] for m in range(5)]
        tangent = [u[1, m, rows, :] for m in range(5)]
        fp, ft = jax.jvp(gradient_fields, (primal,), (tangent,))
        for m in range(4):
            w[0, m, rows, :] = fp[m]
            w[1, m, rows, :] = ft[m]

    fields = w[...].reshape(8 * C, VW)
    for a in range(3):
        q[a] = derive(fields, dh_ref[a], dl_ref[a]).reshape(2, 4, C, VW)

    for copy in zcopies1 + pcopies1:
        copy.wait()
    low_wall = jnp.where(source[2] < 0.0, 1.0, 0.0)
    high_wall = jnp.where(source[3] < 0.0, 1.0, 0.0)
    wall = jnp.where(first, low_wall, high_wall) > 0.5

    def put1(pt, m, a, value):
        if a == 1:
            own = uf[pt, m, a]
            value = jnp.where(wall, own if m % 4 == 0 else -own, value)
        of[pt, m, a] = jnp.where(fnode < 25, value, uf[pt, m, a])

    plane_outside(own1, rb1, 5, put1)
    layer_outside(blocks1, zr1, 5, put1)

    for a in range(3):
        @pl.loop(0, C // 8, unroll=True)
        def _(i):
            rows = pl.ds(pl.multiple_of(i * 8, 8), 8)
            primal = ([uf[0, m, a, rows, :] for m in range(5)], [of[0, m, a, rows, :] for m in range(5)])
            tangent = ([uf[1, m, a, rows, :] for m in range(5)], [of[1, m, a, rows, :] for m in range(5)])
            jp, jt = jax.jvp(jump_fields, primal, tangent)
            for m in range(4):
                jf[a, 0, m, rows, :] = (0.5 * LIFT) * sign * jp[m]
                jf[a, 1, m, rows, :] = (0.5 * LIFT) * sign * jt[m]

        q[a] += left(jf[a].reshape(8 * C, FW), lift_ref[a], 2).reshape(2, 4, C, VW)

    @pl.loop(0, C // 8, unroll=True)
    def _(i):
        rows = pl.ds(pl.multiple_of(i * 8, 8), 8)
        scale = [mv[a, rows, :] for a in range(3)]
        states = [[u[pt, m, rows, :] for m in range(5)] for pt in range(2)]
        grads = [
            [[scale[a] * q[a, pt, m, rows, :] for m in range(4)] for a in range(3)]
            for pt in range(2)
        ]
        vp, vt = jax.jvp(viscous_all, (states[0], grads[0]), (states[1], grads[1]))
        for a in range(3):
            for m in range(4):
                v[a, 0, m, rows, :] = vp[a][m]
                v[a, 1, m, rows, :] = vt[a][m]

    for a in range(3):
        vf[a] = left(v[a].reshape(8 * C, VW), pick_ref[a], 3).reshape(2, 4, C, FW)
    blocks2, table2, sent2, zcopies2 = exchange(
        lambda pt, m, a: vf[a, pt, m], 4, sb2, rb2, zs2, zr2, 4
    )
    pcopies2 = finish_send(sent2, sb2, rb2, 4)
    for copy in pcopies2 + zcopies2:
        copy.start()

    own2 = sum(dot(hot_own, p) for p in table2[::-1])

    @pl.loop(0, C // 8, unroll=True)
    def _(i):
        rows = pl.ds(pl.multiple_of(i * 8, 8), 8)
        states = [[u[pt, m, rows, :] for m in range(5)] for pt in range(2)]
        for a in range(3):
            scale = mv[a, rows, :]
            fluxes = jax.jvp(lambda x: inviscid(x, a), (states[0],), (states[1],))
            for pt in range(2):
                g[a, pt, 0, rows, :] = scale * fluxes[pt][0]
                for m in range(4):
                    g[a, pt, m + 1, rows, :] = scale * (fluxes[pt][m + 1] - v[a, pt, m, rows, :])

    for a in range(3):
        @pl.loop(0, C // 8, unroll=True)
        def _(i):
            rows = pl.ds(pl.multiple_of(i * 8, 8), 8)
            primal = ([uf[0, m, a, rows, :] for m in range(5)], [of[0, m, a, rows, :] for m in range(5)])
            tangent = ([uf[1, m, a, rows, :] for m in range(5)], [of[1, m, a, rows, :] for m in range(5)])
            sp, stt = jax.jvp(
                lambda inner, outer: surface(inner, outer, sign, a), primal, tangent
            )
            for m in range(5):
                s[a, 0, m, rows, :] = sp[m]
                s[a, 1, m, rows, :] = stt[m]

    total = None
    for a in range(3):
        part = derive(g[a].reshape(10 * C, VW), dh_ref[a], dl_ref[a])
        total = part if total is None else total + part
    r[...] = total.reshape(2, 5, C, VW)

    for copy in zcopies2 + pcopies2:
        copy.wait()

    def put2(pt, m, a, value):
        if a == 1:
            value = jnp.where(wall, vf[a, pt, m], value)
        ov[a, pt, m] = value

    plane_outside(own2, rb2, 4, put2)
    layer_outside(blocks2, zr2, 4, put2)
    lifted = None
    for a in range(3):
        for pt in range(2):
            s[a, pt, 0] = mf[a] * s[a, pt, 0]
            for m in range(4):
                jump = ov[a, pt, m] - vf[a, pt, m]
                s[a, pt, m + 1] = mf[a] * (s[a, pt, m + 1] - (0.5 * LIFT) * sign * jump)
        part = left(s[a].reshape(10 * C, FW), lift_ref[a], 2)
        lifted = part if lifted is None else lifted + part
    r[...] += lifted.reshape(2, 5, C, VW)

    def whole_sum(parts):
        acc = parts[0]
        for part in parts[1:]:
            acc = acc + part
        return jnp.sum(jnp.sum(acc, axis=0, keepdims=True), axis=1, keepdims=True)

    pd = whole_sum([r[1, m] * u[1, m] for m in range(5)])
    dd = whole_sum([u[1, m] * u[1, m] for m in range(5)])
    rs = whole_sum([r[0, m] * r[0, m] for m in range(5)])
    mine = ratio(pd, dd)
    rests = [r[1, m] - mine * u[1, m] for m in range(5)]
    rr = whole_sum([x * x for x in rests])
    rd = whole_sum([x * u[1, m] for m, x in enumerate(rests)])
    lane = lax.broadcasted_iota(jnp.int32, (1, 128), 1)
    row = jnp.zeros((1, 128), F32)
    for i, value in enumerate((pd, dd, rs, rr, rd)):
        row = jnp.where(lane == i, value, row)
    st[...] = row
    copies = [
        pltpu.make_async_remote_copy(
            src_ref=st, dst_ref=sta.at[k], send_sem=asend.at[k], recv_sem=arecv.at[k],
            device_id=peer(k), device_id_type=MESH,
        )
        for k in range(1, everyone)
    ]
    for copy in copies:
        copy.start()
    sta[0] = st[...]
    writes = []
    for pt, (part, out) in enumerate([(res, res_hbm), (prod, prod_hbm)]):
        for l in range(L):
            for m in range(5):
                part[:, l, 125 * m : 125 * (m + 1)] = r[pt, m, :, 128 * l : 128 * l + 125]
        writes.append(pltpu.make_async_copy(part, out, store.at[pt]))
        writes[pt].start()
    for copy in copies:
        copy.wait()
    table_ref[...] = sta[...].reshape(everyone, 128)
    for copy in writes:
        copy.wait()


def finish(
    total_count, part_hbm, prod_hbm, d_hbm, table_hbm, res_hbm, basis_hbm, kry_ref,
    res, prod, d, table_ref, basis, sems,
):
    loads = [
        pltpu.make_async_copy(src, dst, sems.at[i])
        for i, (src, dst) in enumerate(
            [(part_hbm, res), (table_hbm, table_ref), (d_hbm, d), (prod_hbm, prod)]
        )
    ]
    for copy in loads:
        copy.start()
    loads[0].wait()
    first = pltpu.make_async_copy(res, res_hbm, sems.at[4])
    first.start()
    for copy in loads[1:]:
        copy.wait()
    lane = lax.broadcasted_iota(jnp.int32, (1, 128), 1)
    table = table_ref[...]
    pd, dd, rs, rr, rd = [
        jnp.sum(jnp.where(lane == i, table, 0.0), axis=1, keepdims=True) for i in range(5)
    ]
    coefficient = jnp.sum(pd, axis=0, keepdims=True) * (1.0 / total_count)
    shift = ratio(pd, dd) - coefficient
    rr = jnp.sum(rr + 2.0 * shift * rd + shift * shift * dd, axis=0, keepdims=True)
    rs = jnp.sum(rs, axis=0, keepdims=True)
    beta = jnp.sqrt(rr * (1.0 / total_count))
    norm = jnp.sqrt(rs * (1.0 / total_count))
    row = jnp.where(lane == 0, coefficient, jnp.where(lane == 1, beta, norm))
    kry_ref[...] = row[0, :3]
    c, inv = coefficient, 1.0 / beta
    basis[...] = (prod[...] - c[:, :, None] * d[...]) * inv[:, :, None]
    second = pltpu.make_async_copy(basis, basis_hbm, sems.at[5])
    second.start()
    first.wait()
    second.wait()


def local(ns, np_, state, direction, metric, face_source, send_rows):
    C, L, width = state.shape
    slots = send_rows.shape[2]
    SP = -(-slots // 8) * 8
    VW, FW = 128 * L, 64 * L
    own = 4 * C
    keys = np.full((1, own + 2 * SP), -7, np.int32)
    side, rest = np.divmod(np.arange(own), 2 * C)
    keys[0, :own] = 4 * (rest % C) + 2 * (rest // C) + side
    keys[0, own : own + slots] = own + np.arange(slots)
    keys[0, own + SP : own + SP + slots] = own + slots + np.arange(slots)
    tiles = 4 * (slots // 8) + -(-4 * (slots % 8) // 8)
    high, low, pick, lift = operators(L)
    operands = (
        state, direction, jnp.transpose(metric, (2, 1, 0)), face_source.T, send_rows,
        *[jnp.asarray(x) for x in (keys, high, low, pick, lift)],
    )
    vmem = lambda *shape: pltpu.VMEM(shape, F32)
    dma = lambda n: pltpu.SemaphoreType.DMA((n,))
    spec = pl.BlockSpec(memory_space=pltpu.VMEM)
    parts, product, table = pl.pallas_call(
        functools.partial(kernel, ns, np_),
        out_shape=(
            jax.ShapeDtypeStruct(state.shape, F32),
            jax.ShapeDtypeStruct(state.shape, F32),
            jax.ShapeDtypeStruct((ns * np_, 128), F32),
        ),
        in_specs=[pl.BlockSpec(memory_space=pltpu.HBM)] * 10,
        out_specs=(pl.BlockSpec(memory_space=pltpu.HBM),) * 2 + (spec,),
        scratch_shapes=[
            vmem(2, 5, C, VW), vmem(2, 5, 3, C, FW), vmem(2, 5, 3, C, FW),
            vmem(2, 4, C, VW), vmem(3, 2, 4, C, FW), vmem(3, 2, 4, C, VW),
            vmem(3, 2, 4, C, VW), vmem(3, 2, 4, C, FW), vmem(3, 2, 4, C, FW),
            vmem(3, 2, 5, C, VW), vmem(3, 2, 5, C, FW), vmem(2, 5, C, VW),
            vmem(3, C, VW), vmem(3, C, FW),
            vmem(2, tiles, 8, FW), vmem(2, tiles, 8, FW), vmem(2, C, 3 * FW), vmem(2, C, 3 * FW),
            vmem(2, tiles, 8, FW), vmem(2, tiles, 8, FW), vmem(2, C, 2 * FW), vmem(2, C, 2 * FW),
            vmem(1, 128), vmem(ns * np_, 1, 128),
            *[pltpu.VMEM(x.shape, x.dtype) for x in operands],
            dma(8), dma(8), dma(ns * np_), dma(ns * np_), dma(10), dma(2), vmem(C, L, width), vmem(C, L, width),
        ],
        compiler_params=pltpu.CompilerParams(
            collective_id=0, has_side_effects=True, vmem_limit_bytes=63 * 1024 * 1024
        ),
        name="navier",
    )(*operands)
    hbm = pl.BlockSpec(memory_space=pltpu.HBM)
    return pl.pallas_call(
        functools.partial(finish, float(state.size * ns * np_)),
        out_shape=(
            jax.ShapeDtypeStruct(state.shape, F32),
            jax.ShapeDtypeStruct(state.shape, F32),
            jax.ShapeDtypeStruct((3,), F32),
        ),
        in_specs=[hbm] * 4,
        out_specs=(hbm, hbm, spec),
        scratch_shapes=[
            vmem(C, L, width), vmem(C, L, width), vmem(C, L, width), vmem(ns * np_, 128),
            vmem(C, L, width), dma(6),
        ],
        compiler_params=pltpu.CompilerParams(vmem_limit_bytes=63 * 1024 * 1024),
        name="finish",
    )(parts, product, direction, table)


def solution(mesh):
    return jax.shard_map(
        functools.partial(local, mesh.shape["stream"], mesh.shape["span"]),
        mesh=mesh,
        in_specs=(
            P("stream", "span", None),
            P("stream", "span", None),
            P("stream", "span", None),
            P("stream", None),
            P("stream", None, None),
        ),
        out_specs=(P("stream", "span", None), P("stream", "span", None), P()),
        check_vma=False,
    )
```
